32 devices in a mesh: cfg: 2 (over y), expert: 4 (over z), ffn: 4 (over x, core).
Axes of the slice: x: 2, y: 2, z: 4, core: 2. Of those that a mesh axis runs over, the one named last changes fastest.
Arguments:
- tokens: bfloat16 [2048, 2048], P(('cfg', 'expert'), 'ffn'), parts along dimension 0, may hold values from -6 to 6
- chosen: int32 [8, 512], P(('cfg', 'expert')), parts along dimension 0, may hold values from 0 to 1023, as said below
- gates: float32 [8, 512], P(('cfg', 'expert')), parts along dimension 0, may hold values from 0.1 to 1
- capacity: int32 [2], P('cfg'), parts along dimension 0, may hold values from 256 to 512
- w_gate: bfloat16 [4, 2048, 1024], P('expert', None, 'ffn'), may hold values from -0.125 to 0.125
- w_up: bfloat16 [4, 2048, 1024], P('expert', None, 'ffn'), may hold values from -0.125 to 0.125
- w_down: bfloat16 [4, 1024, 2048], P('expert', 'ffn'), may hold values from -0.1875 to 0.1875
Outputs:
- mixed: bfloat16 [2048, 2048], P(('cfg', 'expert'), 'ffn'), parts along dimension 0
The draws below stay inside these ranges and needn't reach their ends.
There are 2 independent parts, one for each index of `cfg`. The reference program is written for one: setup_inputs(seed, part) draws one part's arguments, and reference() takes and returns one part's arrays. A program takes and returns all parts, laid end to end along the dimension named above; an argument that names none is the same for every part. Nothing has to cross between parts.
Inputs may be any that keep to these rules, and one draw needn't show every extreme that they name: `chosen`: each row lists 512 different tokens; at most 256 of one row's tokens lie in one aligned block of 256 tokens, and every row has exactly 256 in some block.
All inputs are finite; a program needn't handle non-finite values.
Results may differ from the reference program's by a relative error of at most 0.013.
Values may be sent and summed in bfloat16 or wider, within the bound.
A program may use at most 64 MiB of HBM per device.

```python
import math
import jax
import jax.numpy as jnp
from jax import lax

D = 2048
FF = 1024
TOK_DEV = 256
FF_DEV = 256
EXPERTS = 4
TOKENS = 1024
CAP = 512
N_FFN = 4


def draw_chosen(key, part):
    half_most = CAP // EXPERTS

    def one_expert(expert_key):
        key_counts, key_sources, key_tokens, key_order = jax.random.split(expert_key, 4)
        shifts = jax.random.randint(key_counts, (EXPERTS // 2,), 0, half_most + 1)
        shifts = shifts.at[0].set(half_most)
        paired = jnp.stack([shifts, -shifts], axis=1).reshape(-1)
        source_order = jax.random.permutation(key_sources, EXPERTS)
        counts = jnp.zeros((EXPERTS,), jnp.int32).at[source_order].set((half_most + paired).astype(jnp.int32))
        token_orders = jax.vmap(lambda inner: jax.random.permutation(inner, TOK_DEV))(jax.random.split(key_tokens, EXPERTS))
        ends = jnp.cumsum(counts)
        starts = ends - counts
        positions = jnp.arange(CAP, dtype=jnp.int32)
        source = jnp.sum((positions[:, None] >= ends[None, :]).astype(jnp.int32), axis=1)
        within = positions - starts[source]
        token_ids = source * TOK_DEV + token_orders[source, within]
        shuffle = jax.random.permutation(key_order, CAP)
        return token_ids[shuffle].astype(jnp.int32)
    expert_keys = jax.random.split(jax.random.fold_in(key, 11), EXPERTS)
    return jax.vmap(one_expert)(expert_keys)


def block_scale(rng, shape, pieces, least, largest):
    gain = 1.0
    for axis_at, shards_of in pieces:
        heights = jax.random.uniform(jax.random.fold_in(jax.random.fold_in(rng, 6), axis_at), (shards_of,), jnp.float32, least / len(pieces), largest / len(pieces))
        gain = gain * jnp.repeat(jnp.exp(heights), shape[axis_at] // shards_of).reshape((-1,) + (1,) * (len(shape) - 1 - axis_at))
    return gain


def centred(key, extent, deviation, reach, cuts=(), held_as=jnp.bfloat16):
    drawn = deviation * jax.random.normal(key, extent, jnp.float32)
    if cuts:
        drawn = drawn * block_scale(key, extent, cuts, -0.22, 0.18)
    return jnp.clip(drawn, -reach, reach).astype(held_as)


def setup_inputs(seed: int = 0, part: int = 0) -> dict:
    key_list = jax.random.split(jax.random.key(seed), 8)
    part_keys = jax.random.split(jax.random.fold_in(key_list[7], part), 8)
    tokens = centred(part_keys[0], (TOKENS, D), 1.0, 6.0, ((0, 4), (1, 4)))
    chosen = draw_chosen(jax.random.fold_in(jax.random.fold_in(key_list[7], part), 71), part)
    gates = jnp.clip(jnp.exp(math.log(1.0) - 2.3025851 * jax.random.uniform(part_keys[2], (EXPERTS, CAP), jnp.float32) ** block_scale(part_keys[2], (EXPERTS, CAP), ((0, 4),), -0.2, 0.2)), 0.1, 1.0)
    capacity = jax.random.randint(part_keys[3], (1,), CAP // 2, CAP + 1).astype(jnp.int32)
    w_gate = centred(key_list[4], (EXPERTS, D, FF), D ** -0.5, 0.125, ((0, 4), (2, 4)))
    w_up = centred(key_list[5], (EXPERTS, D, FF), D ** -0.5, 0.125, ((0, 4), (2, 4)))
    w_down = centred(key_list[6], (EXPERTS, FF, D), FF ** -0.5, 0.1875, ((0, 4), (1, 4)))
    return {"tokens": tokens, "chosen": chosen, "gates": gates, "capacity": capacity, "w_gate": w_gate, "w_up": w_up, "w_down": w_down}


def reference(tokens, chosen, gates, capacity, w_gate, w_up, w_down):
    positions = jnp.arange(CAP, dtype=jnp.int32)
    live = jnp.where(positions[None, :] < capacity[0], gates, jnp.zeros_like(gates)).astype(jnp.float32)

    def expert_step(total, item):
        picked_ids, weights, gate_cols, up_cols, down_rows = item
        gathered = jnp.take(tokens, picked_ids, axis=0)
        summed = jnp.zeros((CAP, D), jnp.float32)
        for block in range(N_FFN):
            low_col = block * FF_DEV
            gate_part = jnp.dot(gathered, gate_cols[:, low_col:low_col + FF_DEV], preferred_element_type=jnp.float32)
            up_part = jnp.dot(gathered, up_cols[:, low_col:low_col + FF_DEV], preferred_element_type=jnp.float32)
            hidden = (jax.nn.silu(gate_part) * up_part).astype(jnp.bfloat16)
            partial_value = jnp.dot(hidden, down_rows[low_col:low_col + FF_DEV, :], preferred_element_type=jnp.float32).astype(jnp.bfloat16)
            summed = summed + lax.optimization_barrier(partial_value).astype(jnp.float32)
        contribution = (weights[:, None] * summed).astype(jnp.bfloat16)
        total = total.at[picked_ids].add(lax.optimization_barrier(contribution).astype(jnp.float32))
        return total, None

    start_total = jnp.zeros((TOKENS, D), jnp.float32)
    total, unused = lax.scan(expert_step, start_total, (chosen, live, w_gate, w_up, w_down))
    return total.astype(jnp.bfloat16)
```

```python
import jax
import jax.numpy as jnp
from jax import lax
from jax.experimental import pallas as pl
from jax.experimental.pallas import tpu as pltpu
from jax.sharding import PartitionSpec as P


def shards_general(tokens, chosen, gates, capacity, w_gate, w_up, w_down):
    experts_n = lax.axis_size("expert")
    tok_dev = tokens.shape[0]
    picked_ids = chosen[0]
    listed = picked_ids.shape[0]
    slot_depth = 2 * listed // experts_n
    positions = jnp.arange(listed, dtype=jnp.int32)
    alive_mask = positions < capacity[0]
    weights = jnp.where(alive_mask, gates[0], jnp.zeros_like(gates[0]))
    source = picked_ids // tok_dev
    offset = picked_ids - source * tok_dev
    member = (source[:, None] == jnp.arange(experts_n, dtype=jnp.int32)[None, :]).astype(jnp.int32)
    before = jnp.cumsum(member, axis=0) - member
    rank_in = jnp.sum(before * member, axis=1)
    slot_of = source * slot_depth + rank_in
    wanted = jnp.where(alive_mask, offset, -1)
    request = jnp.full((experts_n * slot_depth,), -1, jnp.int32).at[slot_of].set(wanted)
    requested = lax.all_to_all(
        request.reshape(experts_n, slot_depth), "expert", split_axis=0, concat_axis=0, tiled=True
    ).reshape(-1)
    usable = requested >= 0
    safe_idx = jnp.maximum(requested, 0)
    gate_cols = w_gate[0]
    up_cols = w_up[0]
    down_rows = w_down[0]
    row_block = jnp.where(
        usable[:, None], jnp.take(tokens, safe_idx, axis=0), jnp.zeros((), jnp.bfloat16)
    )
    slots = lax.all_to_all(
        row_block.reshape(experts_n, slot_depth, -1),
        "expert",
        split_axis=0,
        concat_axis=0,
        tiled=True,
    )
    picked = jnp.take(slots.reshape(experts_n * slot_depth, -1), slot_of, axis=0)
    portion = lax.all_gather(picked, "ffn", axis=1, tiled=True)
    gate_next = jnp.dot(portion, gate_cols, preferred_element_type=jnp.float32)
    up_next = jnp.dot(portion, up_cols, preferred_element_type=jnp.float32)
    hidden = (jax.nn.silu(gate_next) * up_next).astype(jnp.bfloat16)
    partial_value = jnp.dot(hidden, down_rows, preferred_element_type=jnp.float32)
    summed = lax.psum_scatter(
        partial_value.astype(jnp.bfloat16), "ffn", scatter_dimension=1, tiled=True
    ).astype(jnp.float32)
    contribution = (weights[:, None] * summed).astype(jnp.bfloat16)
    returned_slots = (
        jnp.zeros((experts_n * slot_depth, contribution.shape[1]), jnp.bfloat16)
        .at[slot_of]
        .set(contribution)
    )
    returned = lax.all_to_all(
        returned_slots.reshape(experts_n, slot_depth, -1),
        "expert",
        split_axis=0,
        concat_axis=0,
        tiled=True,
    )
    returned = returned.reshape(experts_n * slot_depth, -1)
    placement_map = (requested[None, :] == jnp.arange(tok_dev, dtype=jnp.int32)[:, None]).astype(
        jnp.bfloat16
    )
    mixed = jnp.dot(placement_map, returned, preferred_element_type=jnp.float32)
    return mixed.astype(jnp.bfloat16)


LANES = 128
PLAIN = 2
MESH = pl.DeviceIdType.MESH
KINDS = 20
(D_PAIR, D_PEER, D_CROSS, F_PEER, F_FAR, MERGED_A, MERGED_B, X_SAME, X_DIAG, X_MATE,
 Y_SAME, Y_DIAG, Y_MATE, C_PAIR, P_PAIR, P_CROSS, P_PEER, W_IN, W_OUT, IDS) = range(KINDS)


def dot(a, b):
    return jnp.dot(a, b, preferred_element_type=jnp.float32)


def fused(cap_ref, chosen_ref, gates_ref, tok_hbm, wg_ref, wu_ref, wd_ref, out_ref,
          tok, near, pick, pick_pair, put, put_pair, live, ids_pair, rows, merged, merged_in,
          x_in, x_mate, w_in, w_in_mate, w_out, w_out_mate, acc, hid, y_out, y_in, own_sum,
          con, con_in, part_pair, part_cross, part_peer, part_in, own_out,
          send_sem, recv_sem, load_sem):
    block, width = tok.shape
    listed = chosen_ref.shape[1]
    half = listed // 2
    chunks = width // LANES
    ff = wg_ref.shape[1]
    bf16, f32 = jnp.bfloat16, jnp.float32
    z = lax.axis_index("expert")
    f = lax.axis_index("ffn")
    inner = ((z + 1) // 2) % 2
    pair = z + 1 - 2 * (z % 2)
    mirror = 3 - z
    cross = z + 2 - 4 * (z // 2)
    chip, core = f // 2, f % 2
    slot_id = (f, chip * 2 + 1 - core, (1 - chip) * 2 + core, (1 - chip) * 2 + 1 - core)
    mate, same, diag = ({"ffn": slot_id[s]} for s in (1, 2, 3))
    to_pair, to_mirror, to_cross = ({"expert": e} for e in (pair, mirror, cross))
    sources = (z, pair, cross + (mirror - cross) * inner, mirror + (cross - mirror) * inner)

    barrier = pltpu.get_barrier_semaphore()
    for other in (to_pair, to_cross, mate, same, diag):
        pl.semaphore_signal(barrier, inc=1, device_id=other, device_id_type=MESH)

    @pl.when(inner == 1)
    def _():
        pl.semaphore_signal(barrier, inc=1, device_id=to_mirror, device_id_type=MESH)

    def cols(q):
        return slice(q * LANES, (q + 1) * LANES)

    tok_loads = [pltpu.make_async_copy(tok_hbm.at[:, cols(q)], tok.at[:, cols(q)], load_sem.at[12 + q])
                 for q in range(chunks)]
    for load in tok_loads:
        load.start()
    loads = []
    for s in range(4):
        at = pl.ds(pl.multiple_of(slot_id[s] * width, width), width)
        loads.append([
            pltpu.make_async_copy(wg_ref.at[at, :], w_in.at[s, :, 0:ff], load_sem.at[3 * s]),
            pltpu.make_async_copy(wu_ref.at[at, :], w_in.at[s, :, ff:2 * ff], load_sem.at[3 * s + 1]),
            pltpu.make_async_copy(wd_ref.at[:, at], w_out.at[s], load_sem.at[3 * s + 2]),
        ])
    for group in loads:
        for load in group:
            load.start()

    def copy(kind, q):
        first, second = slice(0, half), slice(half, listed)
        src, dst, to = {
            D_PAIR: lambda: (tok.at[:, cols(q)], near.at[q, 0:block], to_pair),
            D_PEER: lambda: (tok.at[:, cols(q)], near.at[q, block:2 * block], to_mirror),
            D_CROSS: lambda: (tok.at[:, cols(q)], near.at[q, 2 * block:3 * block], to_cross),
            F_PEER: lambda: (near.at[q, block:2 * block], near.at[q, block:2 * block], to_pair),
            F_FAR: lambda: (near.at[q, 2 * block:3 * block], near.at[q, 2 * block:3 * block], to_pair),
            MERGED_A: lambda: (merged.at[q, first], merged_in.at[q, first], to_pair),
            MERGED_B: lambda: (merged.at[q, second], merged_in.at[q, second], to_pair),
            X_SAME: lambda: (rows.at[q, first], x_in.at[0, q], same),
            X_DIAG: lambda: (rows.at[q, second], x_in.at[1, q], diag),
            X_MATE: lambda: (rows.at[q, second], x_mate.at[q], mate),
            Y_SAME: lambda: (y_out.at[0, q], y_in.at[0, q], same),
            Y_DIAG: lambda: (y_out.at[1, q], y_in.at[1, q], diag),
            Y_MATE: lambda: (y_out.at[2, q], y_in.at[2, q], mate),
            C_PAIR: lambda: (con.at[q], con_in.at[q], to_pair),
            P_PAIR: lambda: (part_pair.at[q], part_in.at[0, q], to_pair),
            P_CROSS: lambda: (part_cross.at[q], part_in.at[1, q], to_cross),
            P_PEER: lambda: (part_peer.at[q], part_in.at[0, q], to_mirror),
            W_IN: lambda: (w_in.at[q], w_in_mate.at[q ^ 1], mate),
            W_OUT: lambda: (w_out.at[q], w_out_mate.at[q ^ 1], mate),
            IDS: lambda: (chosen_ref, ids_pair, to_pair),
        }[kind]()
        sent = kind * chunks + q
        landed = kind * chunks + (q ^ 1 if kind in (W_IN, W_OUT) else q)
        return pltpu.make_async_remote_copy(
            src_ref=src, dst_ref=dst, send_sem=send_sem.at[sent], recv_sem=recv_sem.at[landed],
            device_id=to, device_id_type=MESH)

    def start(kind, q):
        copy(kind, q).start()

    def got(kind, q):
        copy(kind, q ^ 1 if kind in (W_IN, W_OUT) else q).wait_recv()

    pl.semaphore_wait(barrier, 5 + inner)

    @pl.when(inner == 0)
    def _():
        start(IDS, 0)
        for q in range(chunks):
            tok_loads[q].wait()
            start(D_CROSS, q)
            start(D_PAIR, q)

    @pl.when(inner == 1)
    def _():
        for q in range(chunks):
            tok_loads[q].wait()
            start(D_PEER, q)
            if q < PLAIN:
                start(D_PAIR, q)

    for group in loads:
        for load in group:
            load.wait()
    for s in range(4):
        start(W_IN, s)
    for s in range(4):
        start(W_OUT, s)

    def turned(value):
        other = jnp.concatenate([value[:, half:], value[:, :half]], axis=1)
        return jnp.where(core == 1, other, value)

    def column(ids):
        return jnp.broadcast_to(ids.astype(f32), (LANES, listed)).T.astype(jnp.int32)

    lane = lax.broadcasted_iota(jnp.int32, (listed, LANES), 1)
    token = lax.broadcasted_iota(jnp.int32, (block, listed), 0)

    def mark(dst, ids, blocks):
        ids_col = column(ids)
        for r, source in enumerate(blocks):
            for h in range(block // LANES):
                hit = ids_col == lane + (source * block + h * LANES)
                at = r * block + h * LANES
                dst[:, at:at + LANES] = jnp.where(hit, 1.0, 0.0).astype(bf16)

    def mark_rows(dst, ids, blocks):
        for r, source in enumerate(blocks):
            dst[r] = jnp.where(ids == token + source * block, 1.0, 0.0).astype(bf16)

    ids = turned(chosen_ref[...])
    mark(pick, ids, sources)
    mark_rows(put, ids, sources)
    position = turned(lax.broadcasted_iota(jnp.int32, (1, listed), 1))
    kept = jnp.where(position < cap_ref[0], turned(gates_ref[...]), 0.0)
    live[...] = jnp.broadcast_to(kept, (LANES, listed)).T

    def picked(matrix, q, part, has_pair):
        at = slice(part * half, (part + 1) * half)
        low = 0 if has_pair else block
        return dot(matrix[at, 0:block], tok[:, cols(q)]) + dot(matrix[at, block:], near[q, low:])

    def send_rows(q, first, second):
        rows[q, 0:half] = first().astype(bf16)
        start(X_SAME, q)
        rows[q, half:listed] = second().astype(bf16)
        start(X_DIAG, q)
        start(X_MATE, q)

    def add(q, pieces, slots, begin=False):
        at = slice(q * LANES, (q + 1) * LANES)
        lhs = jnp.concatenate(pieces, axis=1)
        for i, w in enumerate((w_in, w_in_mate)):
            rhs = jnp.concatenate([w[s, at] for s in slots], axis=0)
            out = slice(i * 2 * ff, (i + 1) * 2 * ff)
            if begin:
                acc[:, out] = dot(lhs, rhs)
            else:
                acc[:, out] += dot(lhs, rhs)

    def add_chip(q):
        got(X_MATE, q)
        if q == 0:
            for s in range(4):
                got(W_IN, s)
        add(q, [rows[q, 0:half], x_mate[q]], (0, 1), q == 0)

    def add_across(q):
        got(X_SAME, q)
        got(X_DIAG, q)
        add(q, [x_in[0, q], x_in[1, q]], (2, 3))

    def behind(q):
        if q >= 1:
            add_chip(q - 1)
        if q >= 2:
            add_across(q - 2)

    @pl.when(inner == 1)
    def _():
        got(IDS, 0)
        pair_ids = turned(ids_pair[...])
        mark(pick_pair, pair_ids, (sources[0],) + sources[2:])
        mark_rows(put_pair, pair_ids, (sources[0],) + sources[2:])
        for q in range(chunks):
            got(D_PEER, q)
            if q < PLAIN:
                start(F_PEER, q)
            got(D_CROSS, q)
            if q < PLAIN:
                start(F_FAR, q)
            else:
                for part, kind in ((0, MERGED_A), (1, MERGED_B)):
                    at = slice(part * half, (part + 1) * half)
                    merged[q, at] = picked(pick_pair, q, part, False).astype(bf16)
                    start(kind, q)
            got(D_PAIR, q)
            send_rows(q, lambda: picked(pick, q, 0, True), lambda: picked(pick, q, 1, True))
            behind(q)

    @pl.when(inner == 0)
    def _():
        for q in range(chunks):
            if q < PLAIN:
                got(D_PAIR, q)
                got(F_PEER, q)
                got(F_FAR, q)
                send_rows(q, lambda: picked(pick, q, 0, True), lambda: picked(pick, q, 1, True))
            else:
                def from_pair(part, kind):
                    at = slice(part * half, (part + 1) * half)
                    own = dot(pick[at, 0:block], tok[:, cols(q)])
                    got(kind, q)
                    return own + merged_in[q, at].astype(f32)

                send_rows(q, lambda: from_pair(0, MERGED_A), lambda: from_pair(1, MERGED_B))
            behind(q)

    add_chip(chunks - 1)
    for q in range(max(chunks - 2, 0), chunks):
        add_across(q)

    for i in range(2):
        gate = acc[:, i * 2 * ff:i * 2 * ff + ff]
        up = acc[:, i * 2 * ff + ff:(i + 1) * 2 * ff]
        hid[i] = (gate / (1.0 + jnp.exp(-gate)) * up).astype(bf16)

    def down(q, slots):
        total = None
        for i, w in enumerate((w_out, w_out_mate)):
            part = dot(hid[i], jnp.concatenate([w[s, :, cols(q)] for s in slots], axis=1))
            total = part if total is None else total + part
        return total[:, :LANES], total[:, LANES:]

    for s in range(4):
        got(W_OUT, s)
    for q in range(chunks):
        first, second = down(q, (2, 3))
        y_out[0, q] = first.astype(bf16)
        start(Y_SAME, q)
        y_out[1, q] = second.astype(bf16)
        start(Y_DIAG, q)
    for q in range(chunks):
        first, second = down(q, (0, 1))
        own_sum[q] = first
        y_out[2, q] = second.astype(bf16)
        start(Y_MATE, q)

    def weigh(q):
        got(Y_MATE, q)
        got(Y_SAME, q)
        con[q, 0:half] = (live[0:half] * (own_sum[q] + y_in[0, q].astype(f32))).astype(bf16)
        got(Y_DIAG, q)
        other = y_in[2, q].astype(f32) + y_in[1, q].astype(f32)
        con[q, half:listed] = (live[half:listed] * other).astype(bf16)

    @pl.when(inner == 0)
    def _():
        for q in range(chunks):
            weigh(q)
            start(C_PAIR, q)
            own_out[q] = dot(put[0], con[q])
        for q in range(chunks):
            got(P_PAIR, q)
            got(P_CROSS, q)
            total = own_out[q] + part_in[0, q].astype(f32) + part_in[1, q].astype(f32)
            out_ref[:, cols(q)] = total.astype(bf16)

    @pl.when(inner == 1)
    def _():
        for q in range(chunks):
            weigh(q)
            part_pair[q] = dot(put[1], con[q]).astype(bf16)
            start(P_PAIR, q)
        for q in range(chunks):
            got(C_PAIR, q)
            part_cross[q] = (dot(put[3], con[q]) + dot(put_pair[2], con_in[q])).astype(bf16)
            start(P_CROSS, q)
            part_peer[q] = (dot(put[2], con[q]) + dot(put_pair[1], con_in[q])).astype(bf16)
            start(P_PEER, q)
            own_out[q] = dot(put[0], con[q]) + dot(put_pair[0], con_in[q])
        for q in range(chunks):
            got(P_PEER, q)
            total = own_out[q] + part_in[0, q].astype(f32)
            out_ref[:, cols(q)] = total.astype(bf16)

    def sent(kind, q):
        copy(kind, q).wait_send()

    for q in range(chunks):
        for kind in (X_SAME, X_DIAG, X_MATE, Y_SAME, Y_DIAG, Y_MATE):
            sent(kind, q)
    for s in range(4):
        sent(W_IN, s)
        sent(W_OUT, s)

    @pl.when(inner == 0)
    def _():
        sent(IDS, 0)
        for q in range(chunks):
            for kind in (D_CROSS, D_PAIR, C_PAIR):
                sent(kind, q)

    @pl.when(inner == 1)
    def _():
        for q in range(chunks):
            for kind in (D_PEER, P_PAIR, P_CROSS, P_PEER):
                sent(kind, q)
            for kind in (D_PAIR, F_PEER, F_FAR) if q < PLAIN else (MERGED_A, MERGED_B):
                sent(kind, q)


def shards_fused(tokens, chosen, gates, capacity, w_gate, w_up, w_down):
    block, width = tokens.shape
    listed = chosen.shape[1]
    half = listed // 2
    ff = w_gate.shape[2]
    chunks = width // LANES
    bf16, f32 = jnp.bfloat16, jnp.float32
    vmem = pl.BlockSpec(memory_space=pltpu.VMEM)
    far = pl.BlockSpec(memory_space=pl.ANY)
    return pl.pallas_call(
        fused,
        out_shape=jax.ShapeDtypeStruct(tokens.shape, bf16),
        in_specs=[pl.BlockSpec(memory_space=pltpu.SMEM), vmem, vmem, far, far, far, far],
        out_specs=vmem,
        scratch_shapes=[
            pltpu.VMEM((block, width), bf16),
            pltpu.VMEM((chunks, 3 * block, LANES), bf16),
            pltpu.VMEM((listed, 4 * block), bf16),
            pltpu.VMEM((listed, 3 * block), bf16),
            pltpu.VMEM((4, block, listed), bf16),
            pltpu.VMEM((3, block, listed), bf16),
            pltpu.VMEM((listed, LANES), f32),
            pltpu.VMEM((1, listed), jnp.int32),
            pltpu.VMEM((chunks, listed, LANES), bf16),
            pltpu.VMEM((chunks, listed, LANES), bf16),
            pltpu.VMEM((chunks, listed, LANES), bf16),
            pltpu.VMEM((2, chunks, half, LANES), bf16),
            pltpu.VMEM((chunks, half, LANES), bf16),
            pltpu.VMEM((4, width, 2 * ff), bf16),
            pltpu.VMEM((4, width, 2 * ff), bf16),
            pltpu.VMEM((4, ff, width), bf16),
            pltpu.VMEM((4, ff, width), bf16),
            pltpu.VMEM((half, 4 * ff), f32),
            pltpu.VMEM((2, half, ff), bf16),
            pltpu.VMEM((3, chunks, half, LANES), bf16),
            pltpu.VMEM((3, chunks, half, LANES), bf16),
            pltpu.VMEM((chunks, half, LANES), f32),
            pltpu.VMEM((chunks, listed, LANES), bf16),
            pltpu.VMEM((chunks, listed, LANES), bf16),
            pltpu.VMEM((chunks, block, LANES), bf16),
            pltpu.VMEM((chunks, block, LANES), bf16),
            pltpu.VMEM((chunks, block, LANES), bf16),
            pltpu.VMEM((2, chunks, block, LANES), bf16),
            pltpu.VMEM((chunks, block, LANES), f32),
            pltpu.SemaphoreType.DMA((KINDS * chunks,)),
            pltpu.SemaphoreType.DMA((KINDS * chunks,)),
            pltpu.SemaphoreType.DMA((12 + chunks,)),
        ],
        compiler_params=pltpu.CompilerParams(collective_id=0, has_side_effects=True),
    )(capacity, chosen, gates, tokens, w_gate[0], w_up[0], w_down[0])


def solution(mesh):
    in_specs = (
        P(("cfg", "expert"), "ffn"),
        P(("cfg", "expert"), None),
        P(("cfg", "expert"), None),
        P("cfg"),
        P("expert", None, "ffn"),
        P("expert", None, "ffn"),
        P("expert", "ffn", None),
    )
    out_specs = P(("cfg", "expert"), "ffn")
    small = mesh.shape["expert"] == 4 and mesh.shape["ffn"] == 4
    body = shards_fused if small else shards_general
    return jax.shard_map(body, mesh=mesh, in_specs=in_specs, out_specs=out_specs, check_vma=False)
```

```python
import jax
import jax.numpy as jnp
from jax import lax
from jax.experimental import pallas as pl
from jax.experimental.pallas import tpu as pltpu
from jax.sharding import PartitionSpec as P


def shards_general(tokens, chosen, gates, capacity, w_gate, w_up, w_down):
    experts_n = lax.axis_size("expert")
    tok_dev = tokens.shape[0]
    picked_ids = chosen[0]
    listed = picked_ids.shape[0]
    slot_depth = 2 * listed // experts_n
    positions = jnp.arange(listed, dtype=jnp.int32)
    alive_mask = positions < capacity[0]
    weights = jnp.where(alive_mask, gates[0], jnp.zeros_like(gates[0]))
    source = picked_ids // tok_dev
    offset = picked_ids - source * tok_dev
    member = (source[:, None] == jnp.arange(experts_n, dtype=jnp.int32)[None, :]).astype(jnp.int32)
    before = jnp.cumsum(member, axis=0) - member
    rank_in = jnp.sum(before * member, axis=1)
    slot_of = source * slot_depth + rank_in
    wanted = jnp.where(alive_mask, offset, -1)
    request = jnp.full((experts_n * slot_depth,), -1, jnp.int32).at[slot_of].set(wanted)
    requested = lax.all_to_all(
        request.reshape(experts_n, slot_depth), "expert", split_axis=0, concat_axis=0, tiled=True
    ).reshape(-1)
    usable = requested >= 0
    safe_idx = jnp.maximum(requested, 0)
    gate_cols = w_gate[0]
    up_cols = w_up[0]
    down_rows = w_down[0]
    row_block = jnp.where(
        usable[:, None], jnp.take(tokens, safe_idx, axis=0), jnp.zeros((), jnp.bfloat16)
    )
    slots = lax.all_to_all(
        row_block.reshape(experts_n, slot_depth, -1),
        "expert",
        split_axis=0,
        concat_axis=0,
        tiled=True,
    )
    picked = jnp.take(slots.reshape(experts_n * slot_depth, -1), slot_of, axis=0)
    portion = lax.all_gather(picked, "ffn", axis=1, tiled=True)
    gate_next = jnp.dot(portion, gate_cols, preferred_element_type=jnp.float32)
    up_next = jnp.dot(portion, up_cols, preferred_element_type=jnp.float32)
    hidden = (jax.nn.silu(gate_next) * up_next).astype(jnp.bfloat16)
    partial_value = jnp.dot(hidden, down_rows, preferred_element_type=jnp.float32)
    summed = lax.psum_scatter(
        partial_value.astype(jnp.bfloat16), "ffn", scatter_dimension=1, tiled=True
    ).astype(jnp.float32)
    contribution = (weights[:, None] * summed).astype(jnp.bfloat16)
    returned_slots = (
        jnp.zeros((experts_n * slot_depth, contribution.shape[1]), jnp.bfloat16)
        .at[slot_of]
        .set(contribution)
    )
    returned = lax.all_to_all(
        returned_slots.reshape(experts_n, slot_depth, -1),
        "expert",
        split_axis=0,
        concat_axis=0,
        tiled=True,
    )
    returned = returned.reshape(experts_n * slot_depth, -1)
    placement_map = (requested[None, :] == jnp.arange(tok_dev, dtype=jnp.int32)[:, None]).astype(
        jnp.bfloat16
    )
    mixed = jnp.dot(placement_map, returned, preferred_element_type=jnp.float32)
    return mixed.astype(jnp.bfloat16)


LANES = 128
MESH = pl.DeviceIdType.MESH
KINDS = 20
PIECES = 8
DISPATCH = ("plain", "plain", "plain", "merged")
COMBINE = ("merged", "merged", "merged", "merged")
VMEM_BYTES = 66 * 1000 * 1000
(D_PAIR, D_PEER, D_CROSS, D_FAR, F_PEER, F_FAR, MERGED_A, MERGED_B, X_SAME, X_DIAG, X_MATE,
 Y_SAME, Y_DIAG, Y_MATE, C_FIRST, C_SECOND, P_PAIR, P_CROSS, P_PEER, IDS) = range(KINDS)


def dot(a, b):
    return jnp.dot(a, b, preferred_element_type=jnp.float32)


def fused(cap_hbm, chosen_hbm, gates_hbm, tok_hbm, wg_ref, wu_ref, wd_ref, out_ref,
          cap_ref, chosen_ref, gates_ref, tok, near, pick, pick_pair, put, put_pair, live, ids_pair, rows, merged, merged_in,
          x_in, x_mate, w_in, w_in_mate, w_out, w_out_mate, acc, hid, y_out, y_in, own_sum,
          con, con_in, part_pair, part_cross, part_peer, part_in, own_out,
          send_sem, recv_sem, load_sem, w_send_sem, w_recv_sem):
    block, width = tok.shape
    listed = chosen_ref.shape[1]
    half = listed // 2
    chunks = width // LANES
    ff = wg_ref.shape[1]
    bf16, f32 = jnp.bfloat16, jnp.float32
    z = lax.axis_index("expert")
    f = lax.axis_index("ffn")
    inner = ((z + 1) // 2) % 2
    pair = z + 1 - 2 * (z % 2)
    mirror = 3 - z
    cross = z + 2 - 4 * (z // 2)
    chip, core = f // 2, f % 2
    slot_id = (f, chip * 2 + 1 - core, (1 - chip) * 2 + core, (1 - chip) * 2 + 1 - core)
    mate, same, diag = ({"ffn": slot_id[s]} for s in (1, 2, 3))
    to_pair, to_mirror, to_cross = ({"expert": e} for e in (pair, mirror, cross))
    sources = (z, pair, cross + (mirror - cross) * inner, mirror + (cross - mirror) * inner)

    barrier = pltpu.get_barrier_semaphore()
    for other in (to_pair, to_cross, mate, same, diag):
        pl.semaphore_signal(barrier, inc=1, device_id=other, device_id_type=MESH)

    @pl.when(inner == 1)
    def _():
        pl.semaphore_signal(barrier, inc=1, device_id=to_mirror, device_id_type=MESH)

    def cols(q):
        return slice(q * LANES, (q + 1) * LANES)

    tok_loads = [pltpu.make_async_copy(tok_hbm.at[:, cols(q)], tok.at[:, cols(q)], load_sem.at[12 + q])
                 for q in range(chunks)]
    small_loads = [pltpu.make_async_copy(src, dst, load_sem.at[12 + chunks + i]) for i, (src, dst) in enumerate(
        ((chosen_hbm, chosen_ref), (gates_hbm, gates_ref), (cap_hbm, cap_ref)))]
    for load in small_loads[:1] + tok_loads + small_loads[1:]:
        load.start()
    loads = []
    for s in range(4):
        at = pl.ds(pl.multiple_of(slot_id[s] * width, width), width)
        loads.append([
            pltpu.make_async_copy(wg_ref.at[at, :], w_in.at[s, :, 0:ff], load_sem.at[3 * s]),
            pltpu.make_async_copy(wu_ref.at[at, :], w_in.at[s, :, ff:2 * ff], load_sem.at[3 * s + 1]),
            pltpu.make_async_copy(wd_ref.at[:, at], w_out.at[s], load_sem.at[3 * s + 2]),
        ])
    for group in loads:
        for load in group:
            load.start()

    def copy(kind, q):
        first, second = slice(0, half), slice(half, listed)
        src, dst, to = {
            D_PAIR: lambda: (tok.at[:, cols(q)], near.at[q, 0:block], to_pair),
            D_PEER: lambda: (tok.at[:, cols(q)], near.at[q, block:2 * block], to_mirror),
            D_CROSS: lambda: (tok.at[:, cols(q)], near.at[q, 2 * block:3 * block], to_cross),
            D_FAR: lambda: (tok.at[:, cols(q)], near.at[q, 2 * block:3 * block], to_mirror),
            F_PEER: lambda: (near.at[q, block:2 * block], near.at[q, block:2 * block], to_pair),
            F_FAR: lambda: (near.at[q, 2 * block:3 * block], near.at[q, 2 * block:3 * block], to_pair),
            MERGED_A: lambda: (merged.at[q, first], merged_in.at[q, first], to_pair),
            MERGED_B: lambda: (merged.at[q, second], merged_in.at[q, second], to_pair),
            X_SAME: lambda: (rows.at[q, first], x_in.at[0, q], same),
            X_DIAG: lambda: (rows.at[q, second], x_in.at[1, q], diag),
            X_MATE: lambda: (rows.at[q, second], x_mate.at[q], mate),
            Y_SAME: lambda: (y_out.at[0, q], y_in.at[0, q], same),
            Y_DIAG: lambda: (y_out.at[1, q], y_in.at[1, q], diag),
            Y_MATE: lambda: (y_out.at[2, q], y_in.at[2, q], mate),
            C_FIRST: lambda: (con.at[q, first], con_in.at[q, first], to_pair),
            C_SECOND: lambda: (con.at[q, second], con_in.at[q, second], to_pair),
            P_PAIR: lambda: (part_pair.at[q], part_in.at[0, q], to_pair),
            P_CROSS: lambda: (part_cross.at[q], part_in.at[1, q], to_cross),
            P_PEER: lambda: (part_peer.at[q], part_in.at[2, q], to_mirror),
            IDS: lambda: (chosen_ref, ids_pair, to_pair),
        }[kind]()
        i = kind * chunks + q
        return pltpu.make_async_remote_copy(
            src_ref=src, dst_ref=dst, send_sem=send_sem.at[i], recv_sem=recv_sem.at[i],
            device_id=to, device_id_type=MESH)

    def w_copy(s, q):
        if q < chunks:
            src, dst = w_in.at[s, cols(q)], w_in_mate.at[s ^ 1, cols(q)]
        else:
            src, dst = w_out.at[s], w_out_mate.at[s ^ 1]
        return pltpu.make_async_remote_copy(
            src_ref=src, dst_ref=dst, send_sem=w_send_sem.at[s * (chunks + 1) + q],
            recv_sem=w_recv_sem.at[(s ^ 1) * (chunks + 1) + q], device_id=mate, device_id_type=MESH)

    pieces = []
    for q in range(chunks):
        pieces += [(0, q), (1, q)]
        if q >= 1:
            pieces += [(2, q - 1), (3, q - 1)]
    pieces += [(2, chunks - 1), (3, chunks - 1)] + [(s, chunks) for s in (2, 3, 0, 1)]

    def push(left, number):
        for s, q in left[:number]:
            w_copy(s, q).start()
        return left[number:]

    def push_some(left):
        return push(left, 4)

    def w_got(slots, q):
        for s in slots:
            w_copy(s ^ 1, q).wait_recv()

    def start(kind, q):
        copy(kind, q).start()

    def got(kind, q):
        copy(kind, q).wait_recv()

    def mode(q):
        return DISPATCH[q]

    pl.semaphore_wait(barrier, 5 + inner)

    @pl.when(inner == 0)
    def _():
        small_loads[0].wait()
        start(IDS, 0)
        for q in range(chunks):
            tok_loads[q].wait()
            if mode(q) != "direct":
                start(D_CROSS, q)
                start(D_PAIR, q)

    @pl.when(inner == 1)
    def _():
        for q in range(chunks):
            tok_loads[q].wait()
            start(D_PEER, q)
            if mode(q) != "merged":
                start(D_PAIR, q)
        small_loads[0].wait()

    for group in loads:
        for load in group:
            load.wait()
    for load in small_loads[1:]:
        load.wait()
    pieces = push(pieces, PIECES)

    def turned(value):
        other = jnp.concatenate([value[:, half:], value[:, :half]], axis=1)
        return jnp.where(core == 1, other, value)

    def column(ids):
        return jnp.broadcast_to(ids.astype(f32), (LANES, listed)).T.astype(jnp.int32)

    lane = lax.broadcasted_iota(jnp.int32, (listed, LANES), 1)
    token = lax.broadcasted_iota(jnp.int32, (block, listed), 0)

    def mark(dst, ids, blocks):
        ids_col = column(ids)
        for r, source in enumerate(blocks):
            for h in range(block // LANES):
                hit = ids_col == lane + (source * block + h * LANES)
                at = r * block + h * LANES
                dst[:, at:at + LANES] = jnp.where(hit, 1.0, 0.0).astype(bf16)

    def mark_rows(dst, ids, blocks):
        for r, source in enumerate(blocks):
            dst[r] = jnp.where(ids == token + source * block, 1.0, 0.0).astype(bf16)

    ids = turned(chosen_ref[...])
    mark(pick, ids, sources)
    mark_rows(put, ids, sources)
    position = turned(lax.broadcasted_iota(jnp.int32, (1, listed), 1))
    kept = jnp.where(position < cap_ref[0], turned(gates_ref[...]), 0.0)
    live[...] = jnp.broadcast_to(kept, (LANES, listed)).T

    def picked(matrix, q, part, has_pair):
        at = slice(part * half, (part + 1) * half)
        low = 0 if has_pair else block
        return dot(matrix[at, 0:block], tok[:, cols(q)]) + dot(matrix[at, block:], near[q, low:])

    def send_rows(q, first, second):
        rows[q, 0:half] = first().astype(bf16)
        start(X_SAME, q)
        rows[q, half:listed] = second().astype(bf16)
        start(X_DIAG, q)
        start(X_MATE, q)

    def add(q, pieces, slots, begin=False):
        at = slice(q * LANES, (q + 1) * LANES)
        lhs = jnp.concatenate(pieces, axis=1)
        for i, w in enumerate((w_in, w_in_mate)):
            rhs = jnp.concatenate([w[s, at] for s in slots], axis=0)
            out = slice(i * 2 * ff, (i + 1) * 2 * ff)
            if begin:
                acc[:, out] = dot(lhs, rhs)
            else:
                acc[:, out] += dot(lhs, rhs)

    def add_chip(q):
        got(X_MATE, q)
        w_got((0, 1), q)
        add(q, [rows[q, 0:half], x_mate[q]], (0, 1), q == 0)

    def add_across(q):
        got(X_SAME, q)
        got(X_DIAG, q)
        w_got((2, 3), q)
        add(q, [x_in[0, q], x_in[1, q]], (2, 3))

    def behind(q):
        if q >= 1:
            add_chip(q - 1)
        if q >= 2:
            add_across(q - 2)

    @pl.when(inner == 1)
    def _():
        got(IDS, 0)
        pair_ids = turned(ids_pair[...])
        mark(pick_pair, pair_ids, (sources[0],) + sources[2:])
        mark_rows(put_pair, pair_ids, (sources[0],) + sources[2:])
        left = pieces
        for q in range(chunks):
            got(D_PEER, q)
            if mode(q) != "merged":
                start(F_PEER, q)
            got(D_CROSS, q)
            if mode(q) == "plain":
                start(F_FAR, q)
            elif mode(q) == "merged":
                for part, kind in ((0, MERGED_A), (1, MERGED_B)):
                    at = slice(part * half, (part + 1) * half)
                    merged[q, at] = picked(pick_pair, q, part, False).astype(bf16)
                    start(kind, q)
            got(D_PAIR, q)
            send_rows(q, lambda: picked(pick, q, 0, True), lambda: picked(pick, q, 1, True))
            left = push_some(left)
            behind(q)

    @pl.when(inner == 0)
    def _():
        left = pieces
        for q in range(chunks):
            if mode(q) != "merged":
                got(D_PAIR, q)
                if q == 0:
                    for late in range(chunks):
                        if mode(late) == "direct":
                            start(D_FAR, late)
                            start(D_CROSS, late)
                            start(D_PAIR, late)
                got(F_PEER, q)
                got(F_FAR if mode(q) == "plain" else D_FAR, q)
                send_rows(q, lambda: picked(pick, q, 0, True), lambda: picked(pick, q, 1, True))
            else:
                def from_pair(part, kind):
                    at = slice(part * half, (part + 1) * half)
                    own = dot(pick[at, 0:block], tok[:, cols(q)])
                    got(kind, q)
                    return own + merged_in[q, at].astype(f32)

                send_rows(q, lambda: from_pair(0, MERGED_A), lambda: from_pair(1, MERGED_B))
            left = push_some(left)
            behind(q)

    add_chip(chunks - 1)
    for q in range(max(chunks - 2, 0), chunks):
        add_across(q)

    for i in range(2):
        gate = acc[:, i * 2 * ff:i * 2 * ff + ff]
        up = acc[:, i * 2 * ff + ff:(i + 1) * 2 * ff]
        hid[i] = (gate / (1.0 + jnp.exp(-gate)) * up).astype(bf16)

    def down(q, slots):
        total = None
        for i, w in enumerate((w_out, w_out_mate)):
            part = dot(hid[i], jnp.concatenate([w[s, :, cols(q)] for s in slots], axis=1))
            total = part if total is None else total + part
        return total[:, :LANES], total[:, LANES:]

    w_got((2, 3), chunks)
    for q in range(chunks):
        first, second = down(q, (2, 3))
        y_out[0, q] = first.astype(bf16)
        start(Y_SAME, q)
        y_out[1, q] = second.astype(bf16)
        start(Y_DIAG, q)
    w_got((0, 1), chunks)
    for q in range(chunks):
        first, second = down(q, (0, 1))
        own_sum[q] = first
        y_out[2, q] = second.astype(bf16)
        start(Y_MATE, q)

    def weigh_first(q):
        got(Y_SAME, q)
        con[q, 0:half] = (live[0:half] * (own_sum[q] + y_in[0, q].astype(f32))).astype(bf16)

    def weigh_second(q):
        got(Y_MATE, q)
        got(Y_DIAG, q)
        other = y_in[2, q].astype(f32) + y_in[1, q].astype(f32)
        con[q, half:listed] = (live[half:listed] * other).astype(bf16)

    def spread(q, order):
        for kind, part, slot in order:
            part[q] = dot(put[slot], con[q]).astype(bf16)
            start(kind, q)

    def finish(q, kinds):
        total = own_out[q]
        for kind, slot in kinds:
            got(kind, q)
            total = total + part_in[slot, q].astype(f32)
        out_ref[:, cols(q)] = total.astype(bf16)

    every = ((P_PAIR, 0), (P_CROSS, 1), (P_PEER, 2))

    @pl.when(inner == 0)
    def _():
        for q in range(chunks):
            weigh_first(q)
            if COMBINE[q] == "merged":
                start(C_FIRST, q)
            weigh_second(q)
            if COMBINE[q] == "merged":
                start(C_SECOND, q)
            else:
                spread(q, ((P_PEER, part_peer, 3), (P_CROSS, part_cross, 2), (P_PAIR, part_pair, 1)))
            own_out[q] = dot(put[0], con[q])
        for q in range(chunks):
            finish(q, every[:2] if COMBINE[q] == "merged" else every)

    @pl.when(inner == 1)
    def _():
        for q in range(chunks):
            weigh_first(q)
            weigh_second(q)
            if COMBINE[q] == "merged":
                spread(q, ((P_PAIR, part_pair, 1),))
            else:
                spread(q, ((P_CROSS, part_cross, 3), (P_PEER, part_peer, 2), (P_PAIR, part_pair, 1)))
                own_out[q] = dot(put[0], con[q])
        for q in range(chunks):
            if COMBINE[q] == "merged":
                got(C_FIRST, q)
                got(C_SECOND, q)
                for kind, part, mine, his in ((P_CROSS, part_cross, 3, 2), (P_PEER, part_peer, 2, 1)):
                    part[q] = (dot(put[mine], con[q]) + dot(put_pair[his], con_in[q])).astype(bf16)
                    start(kind, q)
                own_out[q] = dot(put[0], con[q]) + dot(put_pair[0], con_in[q])
        for q in range(chunks):
            finish(q, every[2:] if COMBINE[q] == "merged" else every)

    def sent(kind, q):
        copy(kind, q).wait_send()

    for q in range(chunks):
        for kind in (X_SAME, X_DIAG, X_MATE, Y_SAME, Y_DIAG, Y_MATE):
            sent(kind, q)
    for s in range(4):
        for q in range(chunks + 1):
            w_copy(s, q).wait_send()

    combined = {"merged": ((C_FIRST, C_SECOND), (P_PAIR, P_CROSS, P_PEER)),
                "direct": ((P_PAIR, P_CROSS, P_PEER),) * 2}
    dispatched = {"plain": ((D_CROSS, D_PAIR), (D_PEER, D_PAIR, F_PEER, F_FAR)),
                  "merged": ((D_CROSS, D_PAIR), (D_PEER, MERGED_A, MERGED_B)),
                  "direct": ((D_CROSS, D_PAIR, D_FAR), (D_PEER, D_PAIR, F_PEER))}

    for role in range(2):
        @pl.when(inner == role)
        def _():
            if role == 0:
                sent(IDS, 0)
            for q in range(chunks):
                for kind in dispatched[DISPATCH[q]][role] + combined[COMBINE[q]][role]:
                    sent(kind, q)


def shards_fused(tokens, chosen, gates, capacity, w_gate, w_up, w_down):
    block, width = tokens.shape
    listed = chosen.shape[1]
    half = listed // 2
    ff = w_gate.shape[2]
    chunks = width // LANES
    bf16, f32 = jnp.bfloat16, jnp.float32
    vmem = pl.BlockSpec(memory_space=pltpu.VMEM)
    far = pl.BlockSpec(memory_space=pltpu.HBM)
    return pl.pallas_call(
        fused,
        out_shape=pltpu.VMEM(tokens.shape, bf16),
        in_specs=[far] * 7,
        out_specs=vmem,
        scratch_shapes=[
            pltpu.SMEM((1,), jnp.int32),
            pltpu.VMEM((1, listed), jnp.int32),
            pltpu.VMEM((1, listed), f32),
            pltpu.VMEM((block, width), bf16),
            pltpu.VMEM((chunks, 3 * block, LANES), bf16),
            pltpu.VMEM((listed, 4 * block), bf16),
            pltpu.VMEM((listed, 3 * block), bf16),
            pltpu.VMEM((4, block, listed), bf16),
            pltpu.VMEM((3, block, listed), bf16),
            pltpu.VMEM((listed, LANES), f32),
            pltpu.VMEM((1, listed), jnp.int32),
            pltpu.VMEM((chunks, listed, LANES), bf16),
            pltpu.VMEM((chunks, listed, LANES), bf16),
            pltpu.VMEM((chunks, listed, LANES), bf16),
            pltpu.VMEM((2, chunks, half, LANES), bf16),
            pltpu.VMEM((chunks, half, LANES), bf16),
            pltpu.VMEM((4, width, 2 * ff), bf16),
            pltpu.VMEM((4, width, 2 * ff), bf16),
            pltpu.VMEM((4, ff, width), bf16),
            pltpu.VMEM((4, ff, width), bf16),
            pltpu.VMEM((half, 4 * ff), f32),
            pltpu.VMEM((2, half, ff), bf16),
            pltpu.VMEM((3, chunks, half, LANES), bf16),
            pltpu.VMEM((3, chunks, half, LANES), bf16),
            pltpu.VMEM((chunks, half, LANES), f32),
            pltpu.VMEM((chunks, listed, LANES), bf16),
            pltpu.VMEM((chunks, listed, LANES), bf16),
            pltpu.VMEM((chunks, block, LANES), bf16),
            pltpu.VMEM((chunks, block, LANES), bf16),
            pltpu.VMEM((chunks, block, LANES), bf16),
            pltpu.VMEM((3, chunks, block, LANES), bf16),
            pltpu.VMEM((chunks, block, LANES), f32),
            pltpu.SemaphoreType.DMA((KINDS * chunks,)),
            pltpu.SemaphoreType.DMA((KINDS * chunks,)),
            pltpu.SemaphoreType.DMA((15 + chunks,)),
            pltpu.SemaphoreType.DMA((4 * (chunks + 1),)),
            pltpu.SemaphoreType.DMA((4 * (chunks + 1),)),
        ],
        compiler_params=pltpu.CompilerParams(
            collective_id=0, has_side_effects=True, vmem_limit_bytes=VMEM_BYTES),
    )(capacity, chosen, gates, tokens, w_gate[0], w_up[0], w_down[0])


def solution(mesh):
    in_specs = (
        P(("cfg", "expert"), "ffn"),
        P(("cfg", "expert"), None),
        P(("cfg", "expert"), None),
        P("cfg"),
        P("expert", None, "ffn"),
        P("expert", None, "ffn"),
        P("expert", "ffn", None),
    )
    out_specs = P(("cfg", "expert"), "ffn")
    small = mesh.shape["expert"] == 4 and mesh.shape["ffn"] == 4
    body = shards_fused if small else shards_general
    return jax.shard_map(body, mesh=mesh, in_specs=in_specs, out_specs=out_specs, check_vma=False)
```

```python
import jax
import jax.numpy as jnp
from jax import lax
from jax.experimental import pallas as pl
from jax.experimental.pallas import tpu as pltpu
from jax.sharding import PartitionSpec as P


def shards_general(tokens, chosen, gates, capacity, w_gate, w_up, w_down):
    experts_n = lax.axis_size("expert")
    tok_dev = tokens.shape[0]
    picked_ids = chosen[0]
    listed = picked_ids.shape[0]
    slot_depth = 2 * listed // experts_n
    positions = jnp.arange(listed, dtype=jnp.int32)
    alive_mask = positions < capacity[0]
    weights = jnp.where(alive_mask, gates[0], jnp.zeros_like(gates[0]))
    source = picked_ids // tok_dev
    offset = picked_ids - source * tok_dev
    member = (source[:, None] == jnp.arange(experts_n, dtype=jnp.int32)[None, :]).astype(jnp.int32)
    before = jnp.cumsum(member, axis=0) - member
    rank_in = jnp.sum(before * member, axis=1)
    slot_of = source * slot_depth + rank_in
    wanted = jnp.where(alive_mask, offset, -1)
    request = jnp.full((experts_n * slot_depth,), -1, jnp.int32).at[slot_of].set(wanted)
    requested = lax.all_to_all(
        request.reshape(experts_n, slot_depth), "expert", split_axis=0, concat_axis=0, tiled=True
    ).reshape(-1)
    usable = requested >= 0
    safe_idx = jnp.maximum(requested, 0)
    gate_cols = w_gate[0]
    up_cols = w_up[0]
    down_rows = w_down[0]
    row_block = jnp.where(
        usable[:, None], jnp.take(tokens, safe_idx, axis=0), jnp.zeros((), jnp.bfloat16)
    )
    slots = lax.all_to_all(
        row_block.reshape(experts_n, slot_depth, -1),
        "expert",
        split_axis=0,
        concat_axis=0,
        tiled=True,
    )
    picked = jnp.take(slots.reshape(experts_n * slot_depth, -1), slot_of, axis=0)
    portion = lax.all_gather(picked, "ffn", axis=1, tiled=True)
    gate_next = jnp.dot(portion, gate_cols, preferred_element_type=jnp.float32)
    up_next = jnp.dot(portion, up_cols, preferred_element_type=jnp.float32)
    hidden = (jax.nn.silu(gate_next) * up_next).astype(jnp.bfloat16)
    partial_value = jnp.dot(hidden, down_rows, preferred_element_type=jnp.float32)
    summed = lax.psum_scatter(
        partial_value.astype(jnp.bfloat16), "ffn", scatter_dimension=1, tiled=True
    ).astype(jnp.float32)
    contribution = (weights[:, None] * summed).astype(jnp.bfloat16)
    returned_slots = (
        jnp.zeros((experts_n * slot_depth, contribution.shape[1]), jnp.bfloat16)
        .at[slot_of]
        .set(contribution)
    )
    returned = lax.all_to_all(
        returned_slots.reshape(experts_n, slot_depth, -1),
        "expert",
        split_axis=0,
        concat_axis=0,
        tiled=True,
    )
    returned = returned.reshape(experts_n * slot_depth, -1)
    placement_map = (requested[None, :] == jnp.arange(tok_dev, dtype=jnp.int32)[:, None]).astype(
        jnp.bfloat16
    )
    mixed = jnp.dot(placement_map, returned, preferred_element_type=jnp.float32)
    return mixed.astype(jnp.bfloat16)


LANES = 128
MESH = pl.DeviceIdType.MESH
KINDS = 20
PIECES = 2
DISPATCH = ("plain", "plain", "plain", "merged")
COMBINE = ("merged", "merged", "merged", "merged")
VMEM_BYTES = 66 * 1000 * 1000
(D_PAIR, D_PEER, D_CROSS, D_FAR, F_PEER, F_FAR, MERGED_A, MERGED_B, X_SAME, X_DIAG, X_MATE,
 Y_SAME, Y_DIAG, Y_MATE, C_FIRST, C_SECOND, P_PAIR, P_CROSS, P_PEER, IDS) = range(KINDS)

BOTH = {X_SAME: 0, X_DIAG: 1, X_MATE: 2, Y_SAME: 3, Y_DIAG: 4, Y_MATE: 5}
SENDS = 10
SEND_AT = {**BOTH, D_PAIR: 6, D_PEER: 7, D_CROSS: 7, D_FAR: 9, F_PEER: 8, F_FAR: 9, MERGED_A: 8, MERGED_B: 9,
           C_FIRST: 6, C_SECOND: 7, P_PAIR: 6, P_CROSS: 7, P_PEER: 8, IDS: 8}
RECVS = 12
RECV_AT = {**BOTH, D_PAIR: 6, D_PEER: 7, D_CROSS: 8, D_FAR: 8, F_PEER: 7, F_FAR: 8, MERGED_A: 7, MERGED_B: 8,
           C_FIRST: 9, C_SECOND: 10, P_PAIR: 9, P_CROSS: 10, P_PEER: 11, IDS: RECVS}


def dot(a, b):
    return jnp.dot(a, b, preferred_element_type=jnp.float32)


def fused(cap_hbm, chosen_hbm, gates_hbm, tok_hbm, wg_ref, wu_ref, wd_ref, out_ref,
          cap_ref, chosen_ref, gates_ref, tok, near, pick, pick_pair, put, put_pair, live, ids_pair, rows, merged, merged_in,
          x_in, x_mate, w_in, w_in_mate, w_out, w_out_mate, acc, hid, y_out, y_in, own_sum,
          con, con_in, part_pair, part_cross, part_peer, part_in, own_out,
          send_sem, recv_sem, load_sem, w_send_sem, w_recv_sem):
    block, width = tok.shape
    listed = chosen_ref.shape[1]
    half = listed // 2
    chunks = width // LANES
    ff = wg_ref.shape[2]
    bf16, f32 = jnp.bfloat16, jnp.float32
    z = lax.axis_index("expert")
    f = lax.axis_index("ffn")
    inner = ((z + 1) // 2) % 2
    pair = z + 1 - 2 * (z % 2)
    mirror = 3 - z
    cross = z + 2 - 4 * (z // 2)
    chip, core = f // 2, f % 2
    slot_id = (f, chip * 2 + 1 - core, (1 - chip) * 2 + core, (1 - chip) * 2 + 1 - core)
    mate, same, diag = ({"ffn": slot_id[s]} for s in (1, 2, 3))
    to_pair, to_mirror, to_cross = ({"expert": e} for e in (pair, mirror, cross))
    sources = (z, pair, cross + (mirror - cross) * inner, mirror + (cross - mirror) * inner)

    barrier = pltpu.get_barrier_semaphore()
    for other in (to_pair, to_cross, mate, same, diag):
        pl.semaphore_signal(barrier, inc=1, device_id=other, device_id_type=MESH)

    @pl.when(inner == 1)
    def _():
        pl.semaphore_signal(barrier, inc=1, device_id=to_mirror, device_id_type=MESH)

    def cols(q):
        return slice(q * LANES, (q + 1) * LANES)

    tok_loads = [pltpu.make_async_copy(tok_hbm.at[:, cols(q)], tok.at[:, cols(q)], load_sem.at[q])
                 for q in range(chunks)]
    small_loads = [pltpu.make_async_copy(src, dst, load_sem.at[chunks + i]) for i, (src, dst) in enumerate(
        ((chosen_hbm, chosen_ref), (gates_hbm, gates_ref), (cap_hbm, cap_ref)))]
    for load in small_loads[:1] + tok_loads + small_loads[1:]:
        load.start()
    w_loads = [pltpu.make_async_copy(wg_ref, w_in.at[:, :, 0:ff], load_sem.at[chunks + 3]),
               pltpu.make_async_copy(wu_ref, w_in.at[:, :, ff:2 * ff], load_sem.at[chunks + 4])]
    for s in range(4):
        w_loads.append(pltpu.make_async_copy(
            wd_ref.at[:, s * width:(s + 1) * width], w_out.at[s], load_sem.at[chunks + 5 + s]))
    for load in w_loads:
        load.start()

    def copy(kind, q):
        first, second = slice(0, half), slice(half, listed)
        src, dst, to = {
            D_PAIR: lambda: (tok.at[:, cols(q)], near.at[q, 0:block], to_pair),
            D_PEER: lambda: (tok.at[:, cols(q)], near.at[q, block:2 * block], to_mirror),
            D_CROSS: lambda: (tok.at[:, cols(q)], near.at[q, 2 * block:3 * block], to_cross),
            D_FAR: lambda: (tok.at[:, cols(q)], near.at[q, 2 * block:3 * block], to_mirror),
            F_PEER: lambda: (near.at[q, block:2 * block], near.at[q, block:2 * block], to_pair),
            F_FAR: lambda: (near.at[q, 2 * block:3 * block], near.at[q, 2 * block:3 * block], to_pair),
            MERGED_A: lambda: (merged.at[q, first], merged_in.at[q, first], to_pair),
            MERGED_B: lambda: (merged.at[q, second], merged_in.at[q, second], to_pair),
            X_SAME: lambda: (rows.at[q, first], x_in.at[0, q], same),
            X_DIAG: lambda: (rows.at[q, second], x_in.at[1, q], diag),
            X_MATE: lambda: (rows.at[q, second], x_mate.at[q], mate),
            Y_SAME: lambda: (y_out.at[0, q], y_in.at[0, q], same),
            Y_DIAG: lambda: (y_out.at[1, q], y_in.at[1, q], diag),
            Y_MATE: lambda: (y_out.at[2, q], y_in.at[2, q], mate),
            C_FIRST: lambda: (con.at[q, first], con_in.at[q, first], to_pair),
            C_SECOND: lambda: (con.at[q, second], con_in.at[q, second], to_pair),
            P_PAIR: lambda: (part_pair.at[q], part_in.at[0, q], to_pair),
            P_CROSS: lambda: (part_cross.at[q], part_in.at[1, q], to_cross),
            P_PEER: lambda: (part_peer.at[q], part_in.at[2, q], to_mirror),
            IDS: lambda: (chosen_ref, ids_pair, to_pair),
        }[kind]()
        return pltpu.make_async_remote_copy(
            src_ref=src, dst_ref=dst, send_sem=send_sem.at[SEND_AT[kind] * chunks + q],
            recv_sem=recv_sem.at[RECV_AT[kind] * chunks + q], device_id=to, device_id_type=MESH)

    def w_copy(q):
        if q < chunks:
            src, dst = w_in.at[:, cols(q)], w_in_mate.at[:, cols(q)]
        else:
            src, dst = w_out, w_out_mate
        return pltpu.make_async_remote_copy(
            src_ref=src, dst_ref=dst, send_sem=w_send_sem.at[q], recv_sem=w_recv_sem.at[q],
            device_id=mate, device_id_type=MESH)

    def push(left, number):
        for q in left[:number]:
            w_copy(q).start()
        return left[number:]

    pieces = list(range(chunks + 1))

    def start(kind, q):
        copy(kind, q).start()

    def got(kind, q):
        copy(kind, q).wait_recv()

    def mode(q):
        return DISPATCH[q]

    pl.semaphore_wait(barrier, 5 + inner)

    @pl.when(inner == 0)
    def _():
        small_loads[0].wait()
        start(IDS, 0)
        for q in range(chunks):
            tok_loads[q].wait()
            if mode(q) != "direct":
                start(D_CROSS, q)
                start(D_PAIR, q)

    @pl.when(inner == 1)
    def _():
        for q in range(chunks):
            tok_loads[q].wait()
            start(D_PEER, q)
            if mode(q) != "merged":
                start(D_PAIR, q)
        small_loads[0].wait()

    for load in w_loads:
        load.wait()
    for load in small_loads[1:]:
        load.wait()
    pieces = push(pieces, PIECES)

    def turned(value):
        other = jnp.concatenate([value[:, half:], value[:, :half]], axis=1)
        return jnp.where(core == 1, other, value)

    def column(ids):
        return jnp.broadcast_to(ids.astype(f32), (LANES, listed)).T.astype(jnp.int32)

    lane = lax.broadcasted_iota(jnp.int32, (listed, LANES), 1)
    token = lax.broadcasted_iota(jnp.int32, (block, listed), 0)

    def mark(dst, ids, blocks):
        ids_col = column(ids)
        for r, source in enumerate(blocks):
            for h in range(block // LANES):
                hit = ids_col == lane + (source * block + h * LANES)
                at = r * block + h * LANES
                dst[:, at:at + LANES] = jnp.where(hit, 1.0, 0.0).astype(bf16)

    def mark_rows(dst, ids, blocks):
        for r, source in enumerate(blocks):
            dst[r] = jnp.where(ids == token + source * block, 1.0, 0.0).astype(bf16)

    ids = turned(chosen_ref[...])
    mark(pick, ids, sources)
    mark_rows(put, ids, sources)
    position = turned(lax.broadcasted_iota(jnp.int32, (1, listed), 1))
    kept = jnp.where(position < cap_ref[0], turned(gates_ref[...]), 0.0)
    live[...] = jnp.broadcast_to(kept, (LANES, listed)).T

    def picked(matrix, q, part, has_pair):
        at = slice(part * half, (part + 1) * half)
        low = 0 if has_pair else block
        return dot(matrix[at, 0:block], tok[:, cols(q)]) + dot(matrix[at, block:], near[q, low:])

    def send_rows(q, first, second):
        rows[q, 0:half] = first().astype(bf16)
        start(X_SAME, q)
        rows[q, half:listed] = second().astype(bf16)
        start(X_DIAG, q)
        start(X_MATE, q)

    def add(q, pieces, slots, begin=False):
        at = slice(q * LANES, (q + 1) * LANES)
        lhs = jnp.concatenate(pieces, axis=1)
        for i, w in enumerate((w_in, w_in_mate)):
            rhs = jnp.concatenate([w[slot_id[s], at] for s in slots], axis=0)
            out = slice(i * 2 * ff, (i + 1) * 2 * ff)
            if begin:
                acc[:, out] = dot(lhs, rhs)
            else:
                acc[:, out] += dot(lhs, rhs)

    def add_chip(q):
        got(X_MATE, q)
        w_copy(q).wait_recv()
        add(q, [rows[q, 0:half], x_mate[q]], (0, 1), q == 0)

    def add_across(q):
        got(X_SAME, q)
        got(X_DIAG, q)
        add(q, [x_in[0, q], x_in[1, q]], (2, 3))

    def behind(q):
        if q >= 1:
            add_chip(q - 1)
        if q >= 2:
            add_across(q - 2)

    @pl.when(inner == 1)
    def _():
        got(IDS, 0)
        pair_ids = turned(ids_pair[...])
        mark(pick_pair, pair_ids, (sources[0],) + sources[2:])
        mark_rows(put_pair, pair_ids, (sources[0],) + sources[2:])
        left = pieces
        for q in range(chunks):
            got(D_PEER, q)
            if mode(q) != "merged":
                start(F_PEER, q)
            got(D_CROSS, q)
            if mode(q) == "plain":
                start(F_FAR, q)
            elif mode(q) == "merged":
                for part, kind in ((0, MERGED_A), (1, MERGED_B)):
                    at = slice(part * half, (part + 1) * half)
                    merged[q, at] = picked(pick_pair, q, part, False).astype(bf16)
                    start(kind, q)
            got(D_PAIR, q)
            send_rows(q, lambda: picked(pick, q, 0, True), lambda: picked(pick, q, 1, True))
            left = push(left, 1)
            behind(q)

    @pl.when(inner == 0)
    def _():
        left = pieces
        for q in range(chunks):
            if mode(q) != "merged":
                got(D_PAIR, q)
                if q == 0:
                    for late in range(chunks):
                        if mode(late) == "direct":
                            start(D_FAR, late)
                            start(D_CROSS, late)
                            start(D_PAIR, late)
                got(F_PEER, q)
                got(F_FAR if mode(q) == "plain" else D_FAR, q)
                send_rows(q, lambda: picked(pick, q, 0, True), lambda: picked(pick, q, 1, True))
            else:
                def from_pair(part, kind):
                    at = slice(part * half, (part + 1) * half)
                    own = dot(pick[at, 0:block], tok[:, cols(q)])
                    got(kind, q)
                    return own + merged_in[q, at].astype(f32)

                send_rows(q, lambda: from_pair(0, MERGED_A), lambda: from_pair(1, MERGED_B))
            left = push(left, 1)
            behind(q)

    add_chip(chunks - 1)
    for q in range(max(chunks - 2, 0), chunks):
        add_across(q)

    for i in range(2):
        gate = acc[:, i * 2 * ff:i * 2 * ff + ff]
        up = acc[:, i * 2 * ff + ff:(i + 1) * 2 * ff]
        hid[i] = (gate / (1.0 + jnp.exp(-gate)) * up).astype(bf16)

    def down(q, slots):
        total = None
        for i, w in enumerate((w_out, w_out_mate)):
            part = dot(hid[i], jnp.concatenate([w[slot_id[s], :, cols(q)] for s in slots], axis=1))
            total = part if total is None else total + part
        return total[:, :LANES], total[:, LANES:]

    w_copy(chunks).wait_recv()
    for q in range(chunks):
        first, second = down(q, (2, 3))
        y_out[0, q] = first.astype(bf16)
        y_out[1, q] = second.astype(bf16)
        for value, kinds in ((0, (Y_SAME, Y_DIAG)), (1, (Y_DIAG, Y_SAME))):
            @pl.when(core == value)
            def _():
                for kind in kinds:
                    start(kind, q)
    for q in range(chunks):
        first, second = down(q, (0, 1))
        own_sum[q] = first
        y_out[2, q] = second.astype(bf16)
        start(Y_MATE, q)

    def weigh_first(q):
        got(Y_SAME, q)
        con[q, 0:half] = (live[0:half] * (own_sum[q] + y_in[0, q].astype(f32))).astype(bf16)

    def weigh_second(q):
        got(Y_MATE, q)
        got(Y_DIAG, q)
        other = y_in[2, q].astype(f32) + y_in[1, q].astype(f32)
        con[q, half:listed] = (live[half:listed] * other).astype(bf16)

    combined = {"merged": ((C_FIRST, C_SECOND), (P_PAIR, P_CROSS, P_PEER)),
                "direct": ((P_PAIR, P_CROSS, P_PEER),) * 2}
    dispatched = {"plain": ((D_CROSS, D_PAIR), (D_PEER, D_PAIR, F_PEER, F_FAR)),
                  "merged": ((D_CROSS, D_PAIR), (D_PEER, MERGED_A, MERGED_B)),
                  "direct": ((D_CROSS, D_PAIR, D_FAR), (D_PEER, D_PAIR, F_PEER))}

    def sent(kind, q):
        copy(kind, q).wait_send()

    def sent_first(role):
        if role == 0:
            sent(IDS, 0)
        for q in range(chunks):
            for kind in dispatched[DISPATCH[q]][role]:
                sent(kind, q)

    def sent_early():
        for q in range(chunks):
            for kind in BOTH:
                sent(kind, q)
        for q in range(chunks + 1):
            w_copy(q).wait_send()

    def sent_late(role):
        for q in range(chunks):
            for kind in combined[COMBINE[q]][role]:
                sent(kind, q)

    def spread(q, order):
        for kind, part, slot in order:
            part[q] = dot(put[slot], con[q]).astype(bf16)
            start(kind, q)

    def finish(q, kinds):
        total = own_out[q]
        for kind, slot in kinds:
            got(kind, q)
            total = total + part_in[slot, q].astype(f32)
        out_ref[:, cols(q)] = total.astype(bf16)

    every = ((P_PAIR, 0), (P_CROSS, 1), (P_PEER, 2))

    @pl.when(inner == 0)
    def _():
        sent_first(0)
        for q in range(chunks):
            weigh_first(q)
            if COMBINE[q] == "merged":
                start(C_FIRST, q)
            weigh_second(q)
            if COMBINE[q] == "merged":
                start(C_SECOND, q)
            else:
                spread(q, ((P_PEER, part_peer, 3), (P_CROSS, part_cross, 2), (P_PAIR, part_pair, 1)))
            own_out[q] = dot(put[0], con[q])
        sent_early()
        for q in range(chunks):
            if q == chunks - 1:
                sent_late(0)
            finish(q, every[:2] if COMBINE[q] == "merged" else every)

    @pl.when(inner == 1)
    def _():
        sent_first(1)
        for q in range(chunks):
            weigh_first(q)
            weigh_second(q)
            if COMBINE[q] == "merged":
                spread(q, ((P_PAIR, part_pair, 1),))
            else:
                spread(q, ((P_CROSS, part_cross, 3), (P_PEER, part_peer, 2), (P_PAIR, part_pair, 1)))
                own_out[q] = dot(put[0], con[q])
        for q in range(chunks):
            if COMBINE[q] == "merged":
                got(C_FIRST, q)
                got(C_SECOND, q)
                for kind, part, mine, his in ((P_CROSS, part_cross, 3, 2), (P_PEER, part_peer, 2, 1)):
                    part[q] = (dot(put[mine], con[q]) + dot(put_pair[his], con_in[q])).astype(bf16)
                    start(kind, q)
                own_out[q] = dot(put[0], con[q]) + dot(put_pair[0], con_in[q])
        sent_early()
        for q in range(chunks):
            if q == chunks - 1:
                sent_late(1)
            finish(q, every[2:] if COMBINE[q] == "merged" else every)


def shards_fused(tokens, chosen, gates, capacity, w_gate, w_up, w_down):
    block, width = tokens.shape
    listed = chosen.shape[1]
    half = listed // 2
    ff = w_gate.shape[2]
    chunks = width // LANES
    bf16, f32 = jnp.bfloat16, jnp.float32
    vmem = pl.BlockSpec(memory_space=pltpu.VMEM)
    far = pl.BlockSpec(memory_space=pltpu.HBM)
    return pl.pallas_call(
        fused,
        out_shape=pltpu.VMEM(tokens.shape, bf16),
        in_specs=[far] * 7,
        out_specs=vmem,
        scratch_shapes=[
            pltpu.SMEM((1,), jnp.int32),
            pltpu.VMEM((1, listed), jnp.int32),
            pltpu.VMEM((1, listed), f32),
            pltpu.VMEM((block, width), bf16),
            pltpu.VMEM((chunks, 3 * block, LANES), bf16),
            pltpu.VMEM((listed, 4 * block), bf16),
            pltpu.VMEM((listed, 3 * block), bf16),
            pltpu.VMEM((4, block, listed), bf16),
            pltpu.VMEM((3, block, listed), bf16),
            pltpu.VMEM((listed, LANES), f32),
            pltpu.VMEM((1, listed), jnp.int32),
            pltpu.VMEM((chunks, listed, LANES), bf16),
            pltpu.VMEM((chunks, listed, LANES), bf16),
            pltpu.VMEM((chunks, listed, LANES), bf16),
            pltpu.VMEM((2, chunks, half, LANES), bf16),
            pltpu.VMEM((chunks, half, LANES), bf16),
            pltpu.VMEM((4, width, 2 * ff), bf16),
            pltpu.VMEM((4, width, 2 * ff), bf16),
            pltpu.VMEM((4, ff, width), bf16),
            pltpu.VMEM((4, ff, width), bf16),
            pltpu.VMEM((half, 4 * ff), f32),
            pltpu.VMEM((2, half, ff), bf16),
            pltpu.VMEM((3, chunks, half, LANES), bf16),
            pltpu.VMEM((3, chunks, half, LANES), bf16),
            pltpu.VMEM((chunks, half, LANES), f32),
            pltpu.VMEM((chunks, listed, LANES), bf16),
            pltpu.VMEM((chunks, listed, LANES), bf16),
            pltpu.VMEM((chunks, block, LANES), bf16),
            pltpu.VMEM((chunks, block, LANES), bf16),
            pltpu.VMEM((chunks, block, LANES), bf16),
            pltpu.VMEM((3, chunks, block, LANES), bf16),
            pltpu.VMEM((chunks, block, LANES), f32),
            pltpu.SemaphoreType.DMA((SENDS * chunks,)),
            pltpu.SemaphoreType.DMA((RECVS * chunks + 1,)),
            pltpu.SemaphoreType.DMA((chunks + 9,)),
            pltpu.SemaphoreType.DMA((chunks + 1,)),
            pltpu.SemaphoreType.DMA((chunks + 1,)),
        ],
        compiler_params=pltpu.CompilerParams(
            collective_id=0, has_side_effects=True, vmem_limit_bytes=VMEM_BYTES),
    )(capacity, chosen, gates, tokens, w_gate.reshape(-1, width, ff), w_up.reshape(-1, width, ff), w_down[0])


def solution(mesh):
    in_specs = (
        P(("cfg", "expert"), "ffn"),
        P(("cfg", "expert"), None),
        P(("cfg", "expert"), None),
        P("cfg"),
        P("expert", None, "ffn"),
        P("expert", None, "ffn"),
        P("expert", "ffn", None),
    )
    out_specs = P(("cfg", "expert"), "ffn")
    small = mesh.shape["expert"] == 4 and mesh.shape["ffn"] == 4
    body = shards_fused if small else shards_general
    return jax.shard_map(body, mesh=mesh, in_specs=in_specs, out_specs=out_specs, check_vma=False)
```

```python
import jax
import jax.numpy as jnp
from jax import lax
from jax.experimental import pallas as pl
from jax.experimental.pallas import tpu as pltpu
from jax.sharding import PartitionSpec as P


def shards_general(tokens, chosen, gates, capacity, w_gate, w_up, w_down):
    experts_n = lax.axis_size("expert")
    tok_dev = tokens.shape[0]
    picked_ids = chosen[0]
    listed = picked_ids.shape[0]
    slot_depth = 2 * listed // experts_n
    positions = jnp.arange(listed, dtype=jnp.int32)
    alive_mask = positions < capacity[0]
    weights = jnp.where(alive_mask, gates[0], jnp.zeros_like(gates[0]))
    source = picked_ids // tok_dev
    offset = picked_ids - source * tok_dev
    member = (source[:, None] == jnp.arange(experts_n, dtype=jnp.int32)[None, :]).astype(jnp.int32)
    before = jnp.cumsum(member, axis=0) - member
    rank_in = jnp.sum(before * member, axis=1)
    slot_of = source * slot_depth + rank_in
    wanted = jnp.where(alive_mask, offset, -1)
    request = jnp.full((experts_n * slot_depth,), -1, jnp.int32).at[slot_of].set(wanted)
    requested = lax.all_to_all(
        request.reshape(experts_n, slot_depth), "expert", split_axis=0, concat_axis=0, tiled=True
    ).reshape(-1)
    usable = requested >= 0
    safe_idx = jnp.maximum(requested, 0)
    gate_cols = w_gate[0]
    up_cols = w_up[0]
    down_rows = w_down[0]
    row_block = jnp.where(
        usable[:, None], jnp.take(tokens, safe_idx, axis=0), jnp.zeros((), jnp.bfloat16)
    )
    slots = lax.all_to_all(
        row_block.reshape(experts_n, slot_depth, -1),
        "expert",
        split_axis=0,
        concat_axis=0,
        tiled=True,
    )
    picked = jnp.take(slots.reshape(experts_n * slot_depth, -1), slot_of, axis=0)
    portion = lax.all_gather(picked, "ffn", axis=1, tiled=True)
    gate_next = jnp.dot(portion, gate_cols, preferred_element_type=jnp.float32)
    up_next = jnp.dot(portion, up_cols, preferred_element_type=jnp.float32)
    hidden = (jax.nn.silu(gate_next) * up_next).astype(jnp.bfloat16)
    partial_value = jnp.dot(hidden, down_rows, preferred_element_type=jnp.float32)
    summed = lax.psum_scatter(
        partial_value.astype(jnp.bfloat16), "ffn", scatter_dimension=1, tiled=True
    ).astype(jnp.float32)
    contribution = (weights[:, None] * summed).astype(jnp.bfloat16)
    returned_slots = (
        jnp.zeros((experts_n * slot_depth, contribution.shape[1]), jnp.bfloat16)
        .at[slot_of]
        .set(contribution)
    )
    returned = lax.all_to_all(
        returned_slots.reshape(experts_n, slot_depth, -1),
        "expert",
        split_axis=0,
        concat_axis=0,
        tiled=True,
    )
    returned = returned.reshape(experts_n * slot_depth, -1)
    placement_map = (requested[None, :] == jnp.arange(tok_dev, dtype=jnp.int32)[:, None]).astype(
        jnp.bfloat16
    )
    mixed = jnp.dot(placement_map, returned, preferred_element_type=jnp.float32)
    return mixed.astype(jnp.bfloat16)


LANES = 128
MESH = pl.DeviceIdType.MESH
KINDS = 20
PIECES = 2
DISPATCH = ("plain", "plain", "plain", "merged")
COMBINE = ("merged", "merged", "merged", "merged")
VMEM_BYTES = 66 * 1000 * 1000
(D_PAIR, D_PEER, D_CROSS, D_FAR, F_PEER, F_FAR, MERGED_A, MERGED_B, X_SAME, X_DIAG, X_MATE,
 Y_SAME, Y_DIAG, Y_MATE, C_FIRST, C_SECOND, P_PAIR, P_CROSS, P_PEER, IDS) = range(KINDS)

BOTH = {X_SAME: 0, X_DIAG: 1, X_MATE: 2, Y_SAME: 3, Y_DIAG: 4, Y_MATE: 5}
SENDS = 10
SEND_AT = {**BOTH, D_PAIR: 6, D_PEER: 7, D_CROSS: 7, D_FAR: 9, F_PEER: 8, F_FAR: 9, MERGED_A: 8, MERGED_B: 9,
           C_FIRST: 6, C_SECOND: 7, P_PAIR: 6, P_CROSS: 7, P_PEER: 8, IDS: 8}
RECVS = 12
RECV_AT = {**BOTH, D_PAIR: 6, D_PEER: 7, D_CROSS: 8, D_FAR: 8, F_PEER: 7, F_FAR: 8, MERGED_A: 7, MERGED_B: 8,
           C_FIRST: 9, C_SECOND: 10, P_PAIR: 9, P_CROSS: 10, P_PEER: 11, IDS: RECVS}


def dot(a, b):
    return jnp.dot(a, b, preferred_element_type=jnp.float32)


def fused(cap_hbm, chosen_hbm, gates_hbm, tok_hbm, wg_ref, wu_ref, wd_ref, out_ref,
          cap_ref, chosen_ref, gates_ref, tok, near, pick, pick_pair, put, put_pair, live, ids_pair, rows, merged, merged_in,
          x_in, x_mate, w_in, w_in_mate, w_out, w_out_mate, acc, hid, y_out, y_in, own_sum,
          con, con_in, part_pair, part_cross, part_peer, part_in, own_out,
          send_sem, recv_sem, load_sem, w_send_sem, w_recv_sem):
    block, width = tok.shape
    listed = chosen_ref.shape[1]
    half = listed // 2
    chunks = width // LANES
    ff = wg_ref.shape[2]
    bf16, f32 = jnp.bfloat16, jnp.float32
    z = lax.axis_index("expert")
    f = lax.axis_index("ffn")
    inner = ((z + 1) // 2) % 2
    pair = z + 1 - 2 * (z % 2)
    mirror = 3 - z
    cross = z + 2 - 4 * (z // 2)
    chip, core = f // 2, f % 2
    slot_id = (f, chip * 2 + 1 - core, (1 - chip) * 2 + core, (1 - chip) * 2 + 1 - core)
    mate, same, diag = ({"ffn": slot_id[s]} for s in (1, 2, 3))
    to_pair, to_mirror, to_cross = ({"expert": e} for e in (pair, mirror, cross))
    sources = (z, pair, cross + (mirror - cross) * inner, mirror + (cross - mirror) * inner)

    barrier = pltpu.get_barrier_semaphore()
    for other in (to_pair, to_cross, mate, same, diag):
        pl.semaphore_signal(barrier, inc=1, device_id=other, device_id_type=MESH)

    @pl.when(inner == 1)
    def _():
        pl.semaphore_signal(barrier, inc=1, device_id=to_mirror, device_id_type=MESH)

    def cols(q):
        return slice(q * LANES, (q + 1) * LANES)

    tok_loads = [pltpu.make_async_copy(tok_hbm.at[:, cols(q)], tok.at[:, cols(q)], load_sem.at[q])
                 for q in range(chunks)]
    small_loads = [pltpu.make_async_copy(src, dst, load_sem.at[chunks + i]) for i, (src, dst) in enumerate(
        ((chosen_hbm, chosen_ref), (gates_hbm, gates_ref), (cap_hbm, cap_ref)))]
    for load in small_loads[:1] + tok_loads + small_loads[1:]:
        load.start()
    w_loads = [pltpu.make_async_copy(wg_ref, w_in.at[:, :, 0:ff], load_sem.at[chunks + 3]),
               pltpu.make_async_copy(wu_ref, w_in.at[:, :, ff:2 * ff], load_sem.at[chunks + 4])]
    for s in range(4):
        w_loads.append(pltpu.make_async_copy(
            wd_ref.at[:, s * width:(s + 1) * width], w_out.at[s], load_sem.at[chunks + 5 + s]))
    for load in w_loads:
        load.start()

    def copy(kind, q):
        first, second = slice(0, half), slice(half, listed)
        src, dst, to = {
            D_PAIR: lambda: (tok.at[:, cols(q)], near.at[q, 0:block], to_pair),
            D_PEER: lambda: (tok.at[:, cols(q)], near.at[q, block:2 * block], to_mirror),
            D_CROSS: lambda: (tok.at[:, cols(q)], near.at[q, 2 * block:3 * block], to_cross),
            D_FAR: lambda: (tok.at[:, cols(q)], near.at[q, 2 * block:3 * block], to_mirror),
            F_PEER: lambda: (near.at[q, block:2 * block], near.at[q, block:2 * block], to_pair),
            F_FAR: lambda: (near.at[q, 2 * block:3 * block], near.at[q, 2 * block:3 * block], to_pair),
            MERGED_A: lambda: (merged.at[q, first], merged_in.at[q, first], to_pair),
            MERGED_B: lambda: (merged.at[q, second], merged_in.at[q, second], to_pair),
            X_SAME: lambda: (rows.at[q, first], x_in.at[0, q], same),
            X_DIAG: lambda: (rows.at[q, second], x_in.at[1, q], diag),
            X_MATE: lambda: (rows.at[q, second], x_mate.at[q], mate),
            Y_SAME: lambda: (y_out.at[0, q], y_in.at[0, q], same),
            Y_DIAG: lambda: (y_out.at[1, q], y_in.at[1, q], diag),
            Y_MATE: lambda: (y_out.at[2, q], y_in.at[2, q], mate),
            C_FIRST: lambda: (con.at[q, first], con_in.at[q, first], to_pair),
            C_SECOND: lambda: (con.at[q, second], con_in.at[q, second], to_pair),
            P_PAIR: lambda: (part_pair.at[q], part_in.at[0, q], to_pair),
            P_CROSS: lambda: (part_cross.at[q], part_in.at[1, q], to_cross),
            P_PEER: lambda: (part_peer.at[q], part_in.at[2, q], to_mirror),
            IDS: lambda: (chosen_ref, ids_pair, to_pair),
        }[kind]()
        return pltpu.make_async_remote_copy(
            src_ref=src, dst_ref=dst, send_sem=send_sem.at[SEND_AT[kind] * chunks + q],
            recv_sem=recv_sem.at[RECV_AT[kind] * chunks + q], device_id=to, device_id_type=MESH)

    def w_copy(q):
        if q < chunks:
            src, dst = w_in.at[:, cols(q)], w_in_mate.at[:, cols(q)]
        else:
            src, dst = w_out, w_out_mate
        return pltpu.make_async_remote_copy(
            src_ref=src, dst_ref=dst, send_sem=w_send_sem.at[q], recv_sem=w_recv_sem.at[q],
            device_id=mate, device_id_type=MESH)

    def push(left, number):
        for q in left[:number]:
            w_copy(q).start()
        return left[number:]

    pieces = list(range(chunks + 1))

    def start(kind, q):
        copy(kind, q).start()

    def got(kind, q):
        copy(kind, q).wait_recv()

    def mode(q):
        return DISPATCH[q]

    pl.semaphore_wait(barrier, 5 + inner)

    @pl.when(inner == 0)
    def _():
        small_loads[0].wait()
        start(IDS, 0)
        for q in range(chunks):
            tok_loads[q].wait()
            if mode(q) != "direct":
                start(D_PAIR, q)
                start(D_CROSS, q)

    @pl.when(inner == 1)
    def _():
        for q in range(chunks):
            tok_loads[q].wait()
            start(D_PEER, q)
            if mode(q) != "merged":
                start(D_PAIR, q)
        small_loads[0].wait()

    for load in w_loads:
        load.wait()
    for load in small_loads[1:]:
        load.wait()
    pieces = push(pieces, PIECES)

    def turned(value):
        other = jnp.concatenate([value[:, half:], value[:, :half]], axis=1)
        return jnp.where(core == 1, other, value)

    def column(ids):
        return jnp.broadcast_to(ids.astype(f32), (LANES, listed)).T.astype(jnp.int32)

    lane = lax.broadcasted_iota(jnp.int32, (listed, LANES), 1)
    token = lax.broadcasted_iota(jnp.int32, (block, listed), 0)

    def mark(dst, ids, blocks):
        ids_col = column(ids)
        for r, source in enumerate(blocks):
            for h in range(block // LANES):
                hit = ids_col == lane + (source * block + h * LANES)
                at = r * block + h * LANES
                dst[:, at:at + LANES] = jnp.where(hit, 1.0, 0.0).astype(bf16)

    def mark_rows(dst, ids, blocks):
        for r, source in enumerate(blocks):
            dst[r] = jnp.where(ids == token + source * block, 1.0, 0.0).astype(bf16)

    ids = turned(chosen_ref[...])
    mark(pick, ids, sources)
    mark_rows(put, ids, sources)
    position = turned(lax.broadcasted_iota(jnp.int32, (1, listed), 1))
    kept = jnp.where(position < cap_ref[0], turned(gates_ref[...]), 0.0)
    live[...] = jnp.broadcast_to(kept, (LANES, listed)).T

    def picked(matrix, q, part, has_pair):
        at = slice(part * half, (part + 1) * half)
        low = 0 if has_pair else block
        return dot(matrix[at, 0:block], tok[:, cols(q)]) + dot(matrix[at, block:], near[q, low:])

    def send_rows(q, first, second):
        rows[q, 0:half] = first().astype(bf16)
        start(X_SAME, q)
        rows[q, half:listed] = second().astype(bf16)
        start(X_DIAG, q)
        start(X_MATE, q)

    def add(q, pieces, slots, begin=False):
        at = slice(q * LANES, (q + 1) * LANES)
        lhs = jnp.concatenate(pieces, axis=1)
        for i, w in enumerate((w_in, w_in_mate)):
            rhs = jnp.concatenate([w[slot_id[s], at] for s in slots], axis=0)
            out = slice(i * 2 * ff, (i + 1) * 2 * ff)
            if begin:
                acc[:, out] = dot(lhs, rhs)
            else:
                acc[:, out] += dot(lhs, rhs)

    def add_chip(q):
        got(X_MATE, q)
        w_copy(q).wait_recv()
        add(q, [rows[q, 0:half], x_mate[q]], (0, 1), q == 0)

    def add_across(q):
        got(X_SAME, q)
        got(X_DIAG, q)
        add(q, [x_in[0, q], x_in[1, q]], (2, 3))

    def behind(q):
        if q >= 1:
            add_chip(q - 1)
        if q >= 2:
            add_across(q - 2)

    @pl.when(inner == 1)
    def _():
        got(IDS, 0)
        pair_ids = turned(ids_pair[...])
        mark(pick_pair, pair_ids, (sources[0],) + sources[2:])
        mark_rows(put_pair, pair_ids, (sources[0],) + sources[2:])
        left = pieces
        for q in range(chunks):
            got(D_PEER, q)
            if mode(q) != "merged":
                start(F_PEER, q)
            got(D_CROSS, q)
            if mode(q) == "plain":
                start(F_FAR, q)
            elif mode(q) == "merged":
                for part, kind in ((0, MERGED_A), (1, MERGED_B)):
                    at = slice(part * half, (part + 1) * half)
                    merged[q, at] = picked(pick_pair, q, part, False).astype(bf16)
                    start(kind, q)
            got(D_PAIR, q)
            send_rows(q, lambda: picked(pick, q, 0, True), lambda: picked(pick, q, 1, True))
            left = push(left, 1)
            behind(q)

    @pl.when(inner == 0)
    def _():
        left = pieces
        for q in range(chunks):
            if mode(q) != "merged":
                got(D_PAIR, q)
                if q == 0:
                    for late in range(chunks):
                        if mode(late) == "direct":
                            start(D_FAR, late)
                            start(D_CROSS, late)
                            start(D_PAIR, late)
                got(F_PEER, q)
                got(F_FAR if mode(q) == "plain" else D_FAR, q)
                send_rows(q, lambda: picked(pick, q, 0, True), lambda: picked(pick, q, 1, True))
            else:
                def from_pair(part, kind):
                    at = slice(part * half, (part + 1) * half)
                    own = dot(pick[at, 0:block], tok[:, cols(q)])
                    got(kind, q)
                    return own + merged_in[q, at].astype(f32)

                send_rows(q, lambda: from_pair(0, MERGED_A), lambda: from_pair(1, MERGED_B))
            left = push(left, 1)
            behind(q)

    add_chip(chunks - 1)
    for q in range(max(chunks - 2, 0), chunks):
        add_across(q)

    for i in range(2):
        gate = acc[:, i * 2 * ff:i * 2 * ff + ff]
        up = acc[:, i * 2 * ff + ff:(i + 1) * 2 * ff]
        hid[i] = (gate / (1.0 + jnp.exp(-gate)) * up).astype(bf16)

    def down(q, slots):
        total = None
        for i, w in enumerate((w_out, w_out_mate)):
            part = dot(hid[i], jnp.concatenate([w[slot_id[s], :, cols(q)] for s in slots], axis=1))
            total = part if total is None else total + part
        return total[:, :LANES], total[:, LANES:]

    w_copy(chunks).wait_recv()
    for q in range(chunks):
        first, second = down(q, (2, 3))
        y_out[0, q] = first.astype(bf16)
        y_out[1, q] = second.astype(bf16)
        for value, kinds in ((0, (Y_SAME, Y_DIAG)), (1, (Y_DIAG, Y_SAME))):
            @pl.when(core == value)
            def _():
                for kind in kinds:
                    start(kind, q)
    for q in range(chunks):
        first, second = down(q, (0, 1))
        own_sum[q] = first
        y_out[2, q] = second.astype(bf16)
        start(Y_MATE, q)

    def weigh_first(q):
        got(Y_SAME, q)
        con[q, 0:half] = (live[0:half] * (own_sum[q] + y_in[0, q].astype(f32))).astype(bf16)

    def weigh_second(q):
        got(Y_MATE, q)
        got(Y_DIAG, q)
        other = y_in[2, q].astype(f32) + y_in[1, q].astype(f32)
        con[q, half:listed] = (live[half:listed] * other).astype(bf16)

    combined = {"merged": ((C_FIRST, C_SECOND), (P_PAIR, P_CROSS, P_PEER)),
                "direct": ((P_PAIR, P_CROSS, P_PEER),) * 2}
    dispatched = {"plain": ((D_CROSS, D_PAIR), (D_PEER, D_PAIR, F_PEER, F_FAR)),
                  "merged": ((D_CROSS, D_PAIR), (D_PEER, MERGED_A, MERGED_B)),
                  "direct": ((D_CROSS, D_PAIR, D_FAR), (D_PEER, D_PAIR, F_PEER))}

    def sent(kind, q):
        copy(kind, q).wait_send()

    def sent_first(role):
        if role == 0:
            sent(IDS, 0)
        for q in range(chunks):
            for kind in dispatched[DISPATCH[q]][role]:
                sent(kind, q)

    def sent_early():
        for q in range(chunks):
            for kind in BOTH:
                sent(kind, q)
        for q in range(chunks + 1):
            w_copy(q).wait_send()

    def sent_late(role):
        for q in range(chunks):
            for kind in combined[COMBINE[q]][role]:
                sent(kind, q)

    def spread(q, order):
        for kind, part, slot in order:
            part[q] = dot(put[slot], con[q]).astype(bf16)
            start(kind, q)

    def finish(q, kinds):
        total = own_out[q]
        for kind, slot in kinds:
            got(kind, q)
            total = total + part_in[slot, q].astype(f32)
        out_ref[:, cols(q)] = total.astype(bf16)

    every = ((P_PAIR, 0), (P_CROSS, 1), (P_PEER, 2))

    @pl.when(inner == 0)
    def _():
        sent_first(0)
        for q in range(chunks):
            weigh_first(q)
            if COMBINE[q] == "merged":
                start(C_FIRST, q)
            weigh_second(q)
            if COMBINE[q] == "merged":
                start(C_SECOND, q)
            else:
                spread(q, ((P_PEER, part_peer, 3), (P_CROSS, part_cross, 2), (P_PAIR, part_pair, 1)))
            own_out[q] = dot(put[0], con[q])
        sent_early()
        for q in range(chunks):
            if q == chunks - 1:
                sent_late(0)
            finish(q, every[:2] if COMBINE[q] == "merged" else every)

    @pl.when(inner == 1)
    def _():
        sent_first(1)
        for q in range(chunks):
            weigh_first(q)
            weigh_second(q)
            if COMBINE[q] == "merged":
                spread(q, ((P_PAIR, part_pair, 1),))
            else:
                spread(q, ((P_CROSS, part_cross, 3), (P_PEER, part_peer, 2), (P_PAIR, part_pair, 1)))
                own_out[q] = dot(put[0], con[q])
        for q in range(chunks):
            if COMBINE[q] == "merged":
                got(C_FIRST, q)
                got(C_SECOND, q)
                for kind, part, mine, his in ((P_CROSS, part_cross, 3, 2), (P_PEER, part_peer, 2, 1)):
                    part[q] = (dot(put[mine], con[q]) + dot(put_pair[his], con_in[q])).astype(bf16)
                    start(kind, q)
                own_out[q] = dot(put[0], con[q]) + dot(put_pair[0], con_in[q])
        sent_early()
        for q in range(chunks):
            if q == chunks - 1:
                sent_late(1)
            finish(q, every[2:] if COMBINE[q] == "merged" else every)


def shards_fused(tokens, chosen, gates, capacity, w_gate, w_up, w_down):
    block, width = tokens.shape
    listed = chosen.shape[1]
    half = listed // 2
    ff = w_gate.shape[2]
    chunks = width // LANES
    bf16, f32 = jnp.bfloat16, jnp.float32
    vmem = pl.BlockSpec(memory_space=pltpu.VMEM)
    far = pl.BlockSpec(memory_space=pltpu.HBM)
    return pl.pallas_call(
        fused,
        out_shape=pltpu.VMEM(tokens.shape, bf16),
        in_specs=[far] * 7,
        out_specs=vmem,
        scratch_shapes=[
            pltpu.SMEM((1,), jnp.int32),
            pltpu.VMEM((1, listed), jnp.int32),
            pltpu.VMEM((1, listed), f32),
            pltpu.VMEM((block, width), bf16),
            pltpu.VMEM((chunks, 3 * block, LANES), bf16),
            pltpu.VMEM((listed, 4 * block), bf16),
            pltpu.VMEM((listed, 3 * block), bf16),
            pltpu.VMEM((4, block, listed), bf16),
            pltpu.VMEM((3, block, listed), bf16),
            pltpu.VMEM((listed, LANES), f32),
            pltpu.VMEM((1, listed), jnp.int32),
            pltpu.VMEM((chunks, listed, LANES), bf16),
            pltpu.VMEM((chunks, listed, LANES), bf16),
            pltpu.VMEM((chunks, listed, LANES), bf16),
            pltpu.VMEM((2, chunks, half, LANES), bf16),
            pltpu.VMEM((chunks, half, LANES), bf16),
            pltpu.VMEM((4, width, 2 * ff), bf16),
            pltpu.VMEM((4, width, 2 * ff), bf16),
            pltpu.VMEM((4, ff, width), bf16),
            pltpu.VMEM((4, ff, width), bf16),
            pltpu.VMEM((half, 4 * ff), f32),
            pltpu.VMEM((2, half, ff), bf16),
            pltpu.VMEM((3, chunks, half, LANES), bf16),
            pltpu.VMEM((3, chunks, half, LANES), bf16),
            pltpu.VMEM((chunks, half, LANES), f32),
            pltpu.VMEM((chunks, listed, LANES), bf16),
            pltpu.VMEM((chunks, listed, LANES), bf16),
            pltpu.VMEM((chunks, block, LANES), bf16),
            pltpu.VMEM((chunks, block, LANES), bf16),
            pltpu.VMEM((chunks, block, LANES), bf16),
            pltpu.VMEM((3, chunks, block, LANES), bf16),
            pltpu.VMEM((chunks, block, LANES), f32),
            pltpu.SemaphoreType.DMA((SENDS * chunks,)),
            pltpu.SemaphoreType.DMA((RECVS * chunks + 1,)),
            pltpu.SemaphoreType.DMA((chunks + 9,)),
            pltpu.SemaphoreType.DMA((chunks + 1,)),
            pltpu.SemaphoreType.DMA((chunks + 1,)),
        ],
        compiler_params=pltpu.CompilerParams(
            collective_id=0, has_side_effects=True, vmem_limit_bytes=VMEM_BYTES),
    )(capacity, chosen, gates, tokens, w_gate.reshape(-1, width, ff), w_up.reshape(-1, width, ff), w_down[0])


def solution(mesh):
    in_specs = (
        P(("cfg", "expert"), "ffn"),
        P(("cfg", "expert"), None),
        P(("cfg", "expert"), None),
        P("cfg"),
        P("expert", None, "ffn"),
        P("expert", None, "ffn"),
        P("expert", "ffn", None),
    )
    out_specs = P(("cfg", "expert"), "ffn")
    small = mesh.shape["expert"] == 4 and mesh.shape["ffn"] == 4
    body = shards_fused if small else shards_general
    return jax.shard_map(body, mesh=mesh, in_specs=in_specs, out_specs=out_specs, check_vma=False)
```
